32 devices in a mesh: gx: 4 (over z), gy: 2 (over y), gz: 4 (over x, core).
Axes of the slice: x: 2, y: 2, z: 4, core: 2. Of those that a mesh axis runs over, the one named last changes fastest.
Arguments:
- positions: float32 [3, 8, 4, 32, 128], P(None, 'gx', 'gy', 'gz'), may hold values from 0 to 1
- shield: float32 [8, 4, 32, 128], P('gx', 'gy', 'gz'), may hold values from 0.3 to 1
- width: float32 [8, 4, 32, 128], P('gx', 'gy', 'gz'), may hold values from 0.5 to 2
- hardness: float32 [8, 4, 32, 128], P('gx', 'gy', 'gz'), may hold values from 0.5 to 2
- softness: float32 [8, 4, 32, 128], P('gx', 'gy', 'gz'), may hold values from 0.5 to 2
- coupling: float32 [8, 4, 32, 128], P('gx', 'gy', 'gz'), may hold values from -0.45 to 0.45
- pair_bits: int32 [8, 4, 32], P('gx', 'gy', 'gz'), may hold values from 8192 to 134217727, as said below
- right_side: float32 [4, 8, 4, 32, 128], P(None, 'gx', 'gy', 'gz'), may hold values from -7 to 7
Outputs:
- solution: float32 [4, 8, 4, 32, 128], P(None, 'gx', 'gy', 'gz')
- residual: float32 [4, 8, 4, 32, 128], P(None, 'gx', 'gy', 'gz')
The draws below stay inside these ranges and needn't reach their ends.
Inputs may be any that keep to these rules, and one draw needn't show every extreme that they name: `pair_bits`: bit k of a tile's word stands for the offset with code k as in the reference program; bit 13 is always 1, bits 27 and up are 0, a bit is 0 where the offset leaves the grid, and the lists are symmetric: bit k of tile t equals bit 26 - k of the tile at t plus that offset.
All inputs are finite; a program needn't handle non-finite values.
Results may differ from the reference program's by a relative error of at most 0.0018.
Values sent between devices are 32-bit elements; how exact they have to be, the bound alone decides.
No kernel may reach another device: no remote copies, remote signals or barrier semaphores. Data moves between devices by JAX's collectives and lax.ppermute only.
A program may use at most 128 MiB of HBM per device.

```python
import math
import jax
import jax.numpy as jnp
from jax import lax

TILE = 128
ITERS = 3
NTX = 8
NTY = 4
NTZ = 32


def draw_pair_bits(key, part):
    forward_bits = jax.random.randint(key, (NTX, NTY, NTZ, 13), 0, 2).astype(jnp.int32)
    padded_bits = jnp.pad(forward_bits, ((1, 1), (1, 1), (1, 1), (0, 0)))
    index_first = lax.broadcasted_iota(jnp.int32, (NTX, NTY, NTZ), 0)
    index_second = lax.broadcasted_iota(jnp.int32, (NTX, NTY, NTZ), 1)
    index_third = lax.broadcasted_iota(jnp.int32, (NTX, NTY, NTZ), 2)
    packed = jnp.full((NTX, NTY, NTZ), 1 << 13, jnp.int32)
    for offset_code in range(27):
        shift_first = offset_code // 9 - 1
        shift_second = offset_code // 3 % 3 - 1
        shift_third = offset_code % 3 - 1
        if offset_code > 13:
            inside = (index_first + shift_first >= 0) & (index_first + shift_first < NTX)
            inside = inside & (index_second + shift_second >= 0) & (index_second + shift_second < NTY)
            inside = inside & (index_third + shift_third >= 0) & (index_third + shift_third < NTZ)
            chosen = jnp.where(inside, forward_bits[:, :, :, offset_code - 14], 0)
            packed = packed + chosen * (1 << offset_code)
        elif offset_code < 13:
            chosen = padded_bits[1 + shift_first:1 + shift_first + NTX, 1 + shift_second:1 + shift_second + NTY, 1 + shift_third:1 + shift_third + NTZ, 12 - offset_code]
            packed = packed + chosen * (1 << offset_code)
    return packed


def draw_right_side(key, part):
    rough_key = jax.random.fold_in(key, 11)
    sign_key = jax.random.fold_in(key, 12)
    wave_key = jax.random.fold_in(key, 13)
    phase_key = jax.random.fold_in(key, 14)
    shape = (4, NTX, NTY, NTZ, TILE)
    rough = jnp.clip(jax.random.normal(rough_key, shape, jnp.float32), -4.0, 4.0)
    signs = jnp.where(jax.random.bernoulli(sign_key, 0.5, (4,)), 1.0, -1.0).astype(jnp.float32)
    waves = jax.random.randint(wave_key, (4, 3), 1, 3).astype(jnp.float32)
    phases = jax.random.uniform(phase_key, (4,), jnp.float32, -math.pi, math.pi)
    coord_first = (lax.broadcasted_iota(jnp.float32, (NTX, NTY, NTZ), 0) + 0.5) / NTX
    coord_second = (lax.broadcasted_iota(jnp.float32, (NTX, NTY, NTZ), 1) + 0.5) / NTY
    coord_third = (lax.broadcasted_iota(jnp.float32, (NTX, NTY, NTZ), 2) + 0.5) / NTZ
    phase_field = waves[:, 0, None, None, None] * coord_first[None] + waves[:, 1, None, None, None] * coord_second[None] + waves[:, 2, None, None, None] * coord_third[None]
    phase_field = 2.0 * math.pi * phase_field + phases[:, None, None, None]
    smooth = signs[:, None, None, None] * (1.0 + 0.5 * jnp.cos(phase_field))
    return (rough + smooth[..., None]).astype(jnp.float32)


def level_of(own_key, dims, pieces, low, top_value):
    def one(position, parts):
        steps = jax.random.uniform(jax.random.fold_in(jax.random.fold_in(own_key, 6), position), (parts,), jnp.float32, low / len(pieces), top_value / len(pieces))
        return jnp.repeat(jnp.exp(steps), dims[position] // parts).reshape((-1,) + (1,) * (len(dims) - position - 1))

    factor_of = one(*pieces[0])
    for cut in pieces[1:]:
        factor_of = factor_of * one(*cut)
    return factor_of


def setup_inputs(seed: int = 0) -> dict:
    key_of = jax.random.split(jax.random.key(seed), 9)
    positions = jnp.clip(1.0 * jax.random.uniform(key_of[0], (3, NTX, NTY, NTZ, TILE), jnp.float32) ** level_of(key_of[0], (3, NTX, NTY, NTZ, TILE), ((1, 4), (2, 2), (3, 4)), -0.2, 0.2), 0.0, 1.0)
    shield = jnp.clip(jnp.exp(math.log(1.0) - 1.2039728 * jax.random.uniform(key_of[1], (NTX, NTY, NTZ, TILE), jnp.float32) ** level_of(key_of[1], (NTX, NTY, NTZ, TILE), ((0, 4), (1, 2), (2, 4)), -0.2, 0.2)), 0.3, 1.0)
    width = jnp.clip(jnp.exp(math.log(2.0) - 1.3862944 * jax.random.uniform(key_of[2], (NTX, NTY, NTZ, TILE), jnp.float32) ** level_of(key_of[2], (NTX, NTY, NTZ, TILE), ((0, 4), (1, 2), (2, 4)), -0.2, 0.2)), 0.5, 2.0)
    hardness = jnp.clip(jnp.exp(math.log(2.0) - 1.3862944 * jax.random.uniform(key_of[3], (NTX, NTY, NTZ, TILE), jnp.float32) ** level_of(key_of[3], (NTX, NTY, NTZ, TILE), ((0, 4), (1, 2), (2, 4)), -0.2, 0.2)), 0.5, 2.0)
    softness = jnp.clip(jnp.exp(math.log(2.0) - 1.3862944 * jax.random.uniform(key_of[4], (NTX, NTY, NTZ, TILE), jnp.float32) ** level_of(key_of[4], (NTX, NTY, NTZ, TILE), ((0, 4), (1, 2), (2, 4)), -0.2, 0.2)), 0.5, 2.0)
    coupling = jnp.clip(jax.random.uniform(key_of[5], (NTX, NTY, NTZ, TILE), jnp.float32, -0.45, 0.45) * level_of(key_of[5], (NTX, NTY, NTZ, TILE), ((0, 4), (1, 2), (2, 4)), -0.4, 0.0), -0.45, 0.45)
    pair_bits = draw_pair_bits(jax.random.fold_in(key_of[8], 71), 0)
    right_side = draw_right_side(jax.random.fold_in(key_of[8], 71), 0)
    return dict(positions=positions, shield=shield, width=width, hardness=hardness, softness=softness, coupling=coupling, pair_bits=pair_bits, right_side=right_side)


coulomb_scale = 0.002
response_scale = 0.003

def index_tuple(values):
    return tuple((jnp.asarray(value).astype(jnp.int32) for value in values))

def pair_terms(own_params, partner, offset_code, own_bits):
    shift_first = (offset_code // 9 - 1).astype(jnp.float32)
    shift_second = (offset_code // 3 % 3 - 1).astype(jnp.float32)
    shift_third = (offset_code % 3 - 1).astype(jnp.float32)

    def separation(column, shift):
        return shift + (partner[column][:, None, :] - own_params[column][:, :, None])
    first = separation(0, shift_first)
    second = separation(1, shift_second)
    third = separation(2, shift_third)
    distance = first * first + second * second + third * third
    coulomb = coulomb_scale * lax.rsqrt(distance + own_params[3][:, :, None] * partner[3][:, None, :])
    response = response_scale * jnp.exp(-distance / (own_params[4][:, :, None] + partner[4][:, None, :]))
    listed = jnp.right_shift(own_bits, offset_code) & 1 > 0
    tile_size = own_params.shape[2]
    diagonal_mask = lax.broadcasted_iota(jnp.int32, (tile_size, tile_size), 0) == lax.broadcasted_iota(jnp.int32, (tile_size, tile_size), 1)
    kept = listed[:, None, None] & jnp.logical_not(diagonal_mask[None] & (offset_code == 13))
    empty_pair = jnp.zeros_like(distance)
    return (jnp.where(kept, coulomb, empty_pair).astype(jnp.bfloat16), jnp.where(kept, response, empty_pair).astype(jnp.bfloat16))

def inner(vector, other_vector):
    return lax.optimization_barrier(jnp.sum((vector * other_vector).reshape(2, 2, -1), axis=(0, 2)))

def widen(scalars):
    return jnp.concatenate([scalars, scalars]).reshape(4, 1, 1, 1, 1)

def reference(positions, shield, width, hardness, softness, coupling, pair_bits, right_side):
    tiles_x, tiles_y, tiles_z, tile_size = hardness.shape
    params = jnp.concatenate([positions, shield[None], width[None]], axis=0)
    params_pad = jnp.pad(params, ((0, 0), (1, 1), (1, 1), (1, 1), (0, 0)))
    plane = tiles_y * tiles_z

    def operate(vector):
        vector_pad = jnp.pad(vector, ((0, 0), (1, 1), (1, 1), (1, 1), (0, 0)))

        def slab_terms(slab_index):
            slab_index = slab_index.astype(jnp.int32)
            own_params = lax.dynamic_slice(params_pad, index_tuple((0, slab_index + 1, 1, 1, 0)), (5, 1, tiles_y, tiles_z, tile_size)).reshape(5, plane, tile_size)
            own_bits = lax.dynamic_slice(pair_bits, index_tuple((slab_index, 0, 0)), (1, tiles_y, tiles_z)).reshape(plane)

            def visit(offset_code, carry):
                row_coulomb, row_response, pair_charge, pair_potential = carry
                offset_code = offset_code.astype(jnp.int32)
                start = index_tuple((0, slab_index + offset_code // 9, offset_code // 3 % 3, offset_code % 3, 0))
                partner = lax.dynamic_slice(params_pad, start, (5, 1, tiles_y, tiles_z, tile_size)).reshape(5, plane, tile_size)
                neighbour = lax.dynamic_slice(vector_pad, start, (4, 1, tiles_y, tiles_z, tile_size)).reshape(4, plane, tile_size)
                coulomb, response = pair_terms(own_params, partner, offset_code, own_bits)
                coulomb = coulomb.astype(jnp.float32)
                response = response.astype(jnp.float32)
                row_coulomb = row_coulomb + lax.optimization_barrier(jnp.sum(coulomb, axis=2))
                row_response = row_response + lax.optimization_barrier(jnp.sum(response, axis=2))
                pair_charge = pair_charge + jnp.einsum('tij,ftj->fti', coulomb, neighbour[:2], precision=lax.Precision.HIGHEST)
                pair_potential = pair_potential + jnp.einsum('tij,ftj->fti', response, neighbour[2:], precision=lax.Precision.HIGHEST)
                return (row_coulomb, row_response, pair_charge, pair_potential)
            flat_zeros = jnp.zeros((plane, tile_size), jnp.float32)
            pair_zeros = jnp.zeros((2, plane, tile_size), jnp.float32)
            return lax.fori_loop(0, 27, visit, (flat_zeros, flat_zeros, pair_zeros, pair_zeros))
        row_coulomb, row_response, pair_charge, pair_potential = lax.map(slab_terms, jnp.arange(tiles_x, dtype=jnp.int32))
        grid = (tiles_x, tiles_y, tiles_z, tile_size)
        row_coulomb = row_coulomb.reshape(grid)
        row_response = row_response.reshape(grid)
        pair_charge = pair_charge.transpose(1, 0, 2, 3).reshape((2,) + grid)
        pair_potential = pair_potential.transpose(1, 0, 2, 3).reshape((2,) + grid)
        image_charge = (hardness + row_coulomb) * vector[:2] + pair_charge + coupling * vector[2:]
        image_potential = (softness + row_response) * vector[2:] - pair_potential + coupling * vector[:2]
        return jnp.concatenate([image_charge, image_potential], axis=0)
    solution = jnp.zeros_like(right_side)
    remainder = right_side
    direction = right_side
    norm_now = inner(remainder, remainder)
    for iteration in range(ITERS):
        applied = operate(direction)
        step_size = norm_now / inner(direction, applied)
        solution = solution + widen(step_size) * direction
        remainder = remainder - widen(step_size) * applied
        norm_next = inner(remainder, remainder)
        direction = remainder + widen(norm_next / norm_now) * direction
        norm_now = norm_next
    residual = right_side - operate(solution)
    return (solution, residual)
```

```python
import math

import jax
import jax.numpy as jnp
import numpy as np
from jax import lax
from jax.experimental import pallas as pl
from jax.experimental.pallas import tpu as pltpu
from jax.sharding import PartitionSpec as P

ITERS = 3

coulomb_scale = 0.002
response_scale = 0.003
length_scale = 1.0 / coulomb_scale
width_scale = -math.log(2.0) * length_scale * length_scale

SHIFT = 3.0

AXES = ("gx", "gy", "gz")
HALO_ORDER = (("gz", 2), ("gx", 0), ("gy", 1))
PARTS = 3
SELF = 13
BUILD_SLOTS = 4
BUILD_RING = 4
APPLY_CHUNK = 8
APPLY_COPY = 2
APPLY_RING = 10


class Piece:
    def __init__(self, array, boxes):
        self.array = array
        self.boxes = boxes

    def face(self, dim, level):
        rows, boxes = [], []
        offset = 0
        for origin, shape in self.boxes:
            volume = shape[0] * shape[1] * shape[2]
            if origin[dim] <= level < origin[dim] + shape[dim]:
                part = self.array[:, offset : offset + volume]
                part = part.reshape((part.shape[0],) + shape + part.shape[2:])
                part = lax.slice_in_dim(part, level - origin[dim], level - origin[dim] + 1, axis=dim + 1)
                cut = tuple(1 if d == dim else shape[d] for d in range(3))
                rows.append(part.reshape(part.shape[0], -1, part.shape[-1]))
                boxes.append((tuple(level if d == dim else origin[d] for d in range(3)), cut))
            offset += volume
        return rows, boxes


def whole_face(pieces, dim, level):
    rows, boxes = [], []
    for piece in pieces:
        more_rows, more_boxes = piece.face(dim, level)
        rows += more_rows
        boxes += more_boxes
    return (jnp.concatenate(rows, axis=1) if len(rows) > 1 else rows[0]), boxes


def moved(boxes, dim, level):
    return [(tuple(level if d == dim else o[d] for d in range(3)), s) for o, s in boxes]


def extended(block, extent):
    pieces = [Piece(block, [((0, 0, 0), extent)])]
    for axis, dim in HALO_ORDER:
        count = lax.axis_size(axis)
        if count == 1:
            continue
        size = extent[dim]
        first, boxes = whole_face(pieces, dim, 0)
        last, _ = whole_face(pieces, dim, size - 1)
        if count == 2:
            sent = jnp.where(lax.axis_index(axis) == 0, last, first)
            got = lax.ppermute(sent, axis, [(0, 1), (1, 0)])
            pieces = pieces + [Piece(got, moved(boxes, dim, size))]
        else:
            forward = [(i, (i + 1) % count) for i in range(count)]
            backward = [(target, source) for source, target in forward]
            low = lax.ppermute(last, axis, forward)
            high = lax.ppermute(first, axis, backward)
            pieces = pieces + [
                Piece(low, moved(boxes, dim, -1)),
                Piece(high, moved(boxes, dim, size)),
            ]
    joined = jnp.concatenate([piece.array for piece in pieces], axis=1)
    return joined, [box for piece in pieces for box in piece.boxes]


def storage_rows(boxes, extent, counts):
    rows = {}
    offset = 0
    for origin, shape in boxes:
        for a in range(shape[0]):
            for b in range(shape[1]):
                for c in range(shape[2]):
                    rows[(origin[0] + a, origin[1] + b, origin[2] + c)] = offset
                    offset += 1

    def row_of(coord):
        fixed = list(coord)
        for axis, dim in HALO_ORDER:
            outside = not 0 <= fixed[dim] < extent[dim]
            if outside and counts[axis] == 1:
                fixed[dim] = 0
            elif outside and counts[axis] == 2:
                fixed[dim] = extent[dim]
        return rows[tuple(fixed)]

    return row_of


def candidate_table(boxes, extent, counts):
    row_of = storage_rows(boxes, extent, counts)
    table = []
    for x in range(extent[0]):
        for y in range(extent[1]):
            for z in range(extent[2]):
                own = (x * extent[1] + y) * extent[2] + z
                for a in range(3):
                    for b in range(3):
                        for c in range(3):
                            partner = row_of((x + a - 1, y + b - 1, z + c - 1))
                            assert own < 255 and partner < 256
                            table.append(own | a << 8 | b << 10 | c << 12 | partner << 14)
    return np.asarray(table, np.int32)


def list_kernel(bits_ref, table_ref, list_ref, count_ref):
    tiles = bits_ref.shape[0]
    pad = list_ref.shape[0] - 27 * tiles

    def visit(tile, filled):
        word = bits_ref[tile]
        list_ref[tile] = table_ref[tile * 27 + SELF]
        for code in range(27):
            if code != SELF:
                list_ref[filled] = table_ref[tile * 27 + code]
                filled = filled + ((word >> code) & 1)
        return filled

    filled = lax.fori_loop(0, tiles, visit, jnp.int32(tiles))
    for extra in range(pad):
        list_ref[filled + extra] = tiles
    count_ref[0] = filled


def split_rows(values):
    parts = []
    rest = values
    for _ in range(PARTS):
        part = rest.astype(jnp.bfloat16).astype(jnp.float32)
        parts.append(part)
        rest = rest - part
    return parts


def fill_vectors(source_ref, first_row, rows_all, vec_ref):
    def one(tile, carry):
        values = source_ref[pl.ds(first_row + tile, 4, stride=rows_all), :]
        parts = split_rows(values)
        stacked = jnp.concatenate(parts + [jnp.ones_like(values)], axis=0)
        vec_ref[tile] = stacked.astype(jnp.bfloat16)
        return carry

    lax.fori_loop(0, rows_all, one, 0, unroll=8)


def pair_parts(total):
    joined = total[0:4] + total[4:8] + total[8:12]
    return joined[0:2, 0:128], joined[2:4, 128:256]


def image_rows(values, pair_charge, pair_potential, diag_charge, diag_potential, linking):
    charge, potential = values[0:2], values[2:4]
    image_charge = diag_charge * charge + pair_charge + linking * potential
    image_potential = diag_potential * potential - pair_potential + linking * charge
    return jnp.concatenate([image_charge, image_potential], axis=0)


def block_product(vectors, block):
    return lax.dot_general(vectors, block, (((1,), (1,)), ((), ())), preferred_element_type=jnp.float32)


def build_kernel(list_ref, count_ref, joined_ref, own_ref, hard_ref, soft_ref, link_ref,
                 store_ref, diag_charge_ref, diag_potential_ref, image_ref,
                 row_ref, spread_ref, vec_ref, sum_ref, even_ref, odd_ref, sems):
    tiles = hard_ref.shape[0]
    rows_all = vec_ref.shape[0]
    size = hard_ref.shape[1]
    count = count_ref[0]

    field = lax.broadcasted_iota(jnp.int32, (8, size), 0)
    scale = jnp.where(field < 4, jnp.float32(length_scale), jnp.float32(width_scale))

    def prepare(tile, carry):
        row_ref[tile] = joined_ref[pl.ds(tile, 8, stride=rows_all), :] * scale
        return carry

    lax.fori_loop(0, rows_all, prepare, 0, unroll=8)
    fill_vectors(joined_ref, 5 * rows_all, rows_all, vec_ref)

    line = lax.broadcasted_iota(jnp.int32, (32, 5 * size), 0)
    chosen = lax.broadcasted_iota(jnp.int32, (32, 5 * size), 1) // size
    select = jnp.where(((line & 7) == chosen) & (line < 24), 1.0, 0.0).astype(jnp.bfloat16)

    def spread(tile, carry):
        params = row_ref[tile]
        stacked = jnp.concatenate(split_rows(params) + [jnp.zeros_like(params)], axis=0)
        spread_ref[tile] = lax.dot_general(
            stacked.astype(jnp.bfloat16), select, (((0,), (0,)), ((), ())), preferred_element_type=jnp.float32)
        sum_ref[tile] = jnp.zeros(sum_ref.shape[1:], jnp.float32)
        return carry

    lax.fori_loop(0, tiles, spread, 0, unroll=2)
    sum_ref[tiles] = jnp.zeros(sum_ref.shape[1:], jnp.float32)

    def multiply(ring_ref, base, entries):
        for slot, entry in enumerate(entries):
            product = block_product(vec_ref[(entry >> 14) & 255], ring_ref[base, slot])
            tile = entry & 255
            sum_ref[tile] = sum_ref[tile] + product

    def out_copy(ring_ref, half, base, first):
        return pltpu.make_async_copy(
            ring_ref.at[base], store_ref.at[pl.ds(first, BUILD_SLOTS)], sems.at[half, base])

    def pair_block(ring_ref, base, slot, entry, own_pairs):
        own = jnp.minimum(entry & 255, tiles - 1)
        partner = (entry >> 14) & 255
        shift_a = (((entry >> 8) & 3) - 1).astype(jnp.float32) * length_scale
        shift_b = (((entry >> 10) & 3) - 1).astype(jnp.float32) * length_scale
        shift_c = (((entry >> 12) & 3) - 1).astype(jnp.float32) * length_scale
        theirs = row_ref[partner]
        full = (16, size)
        their_a = jnp.broadcast_to(theirs[0:1] + shift_a, full)
        their_b = jnp.broadcast_to(theirs[1:2] + shift_b, full)
        their_c = jnp.broadcast_to(theirs[2:3] + shift_c, full)
        their_shield = jnp.broadcast_to(theirs[3:4], full)
        their_width = jnp.broadcast_to(theirs[4:5], full)
        for group in range(size // 16):
            rows = slice(16 * group, 16 * group + 16)

            def mine(c):
                return spread_ref[own, rows, c * size : (c + 1) * size]

            delta_a = their_a - mine(0)
            delta_b = their_b - mine(1)
            delta_c = their_c - mine(2)
            distance = delta_a * delta_a + delta_b * delta_b + delta_c * delta_c
            coulomb = lax.rsqrt(distance + mine(3) * their_shield)
            response = response_scale * jnp.exp2(distance / (mine(4) + their_width))
            if own_pairs:
                line = lax.broadcasted_iota(jnp.int32, full, 0) + 16 * group
                other = line != lax.broadcasted_iota(jnp.int32, full, 1)
                coulomb = jnp.where(other, coulomb, 0.0)
                response = jnp.where(other, response, 0.0)
            ring_ref[base, slot, rows, :] = coulomb.astype(jnp.bfloat16)
            ring_ref[base, slot, size + 16 * group : size + 16 * group + 16, :] = response.astype(jnp.bfloat16)

    span = 2 * BUILD_SLOTS

    def entries_at(first):
        return [list_ref[first + slot] for slot in range(BUILD_SLOTS)]

    def turns(first, last, own_pairs):
        def visit(turn, carry):
            base = lax.rem(turn, BUILD_RING)
            before = lax.rem(turn + BUILD_RING - 1, BUILD_RING)
            start = turn * span

            @pl.when(turn >= BUILD_RING)
            def _():
                out_copy(even_ref, 0, base, 0).wait()
                out_copy(odd_ref, 1, base, 0).wait()

            late = [
                jnp.where(turn > 0, list_ref[jnp.maximum(start - BUILD_SLOTS + slot, 0)], tiles)
                for slot in range(BUILD_SLOTS)
            ]
            even, odd = entries_at(start), entries_at(start + BUILD_SLOTS)
            multiply(odd_ref, before, late)
            for slot, entry in enumerate(even):
                pair_block(even_ref, base, slot, entry, own_pairs)
            multiply(even_ref, base, even)
            for slot, entry in enumerate(odd):
                pair_block(odd_ref, base, slot, entry, own_pairs)
            out_copy(even_ref, 0, base, start).start()
            out_copy(odd_ref, 1, base, start + BUILD_SLOTS).start()
            return carry

        lax.fori_loop(first, last, visit, 0)

    assert tiles % span == 0
    own_turns = tiles // span
    all_turns = (count + span - 1) // span
    turns(0, own_turns, True)
    turns(own_turns, all_turns, False)
    final = all_turns - 1
    multiply(odd_ref, lax.rem(final, BUILD_RING), entries_at(final * span + BUILD_SLOTS))
    for group in range(BUILD_RING):
        @pl.when(group < all_turns)
        def _():
            out_copy(even_ref, 0, group, 0).wait()
            out_copy(odd_ref, 1, group, 0).wait()

    def finish(tile, carry):
        total = sum_ref[tile]
        one = pl.ds(tile, 1)
        diag_charge = hard_ref[one, :] + total[12:13, 0:128] - SHIFT
        diag_potential = soft_ref[one, :] + total[12:13, 128:256] - SHIFT
        diag_charge_ref[one, :] = diag_charge
        diag_potential_ref[one, :] = diag_potential
        values = own_ref[pl.ds(tile, 4, stride=tiles), :]
        pair_charge, pair_potential = pair_parts(total)
        image_ref[pl.ds(tile, 4, stride=tiles), :] = image_rows(
            values, pair_charge, pair_potential, diag_charge, diag_potential, link_ref[one, :])
        return carry

    lax.fori_loop(0, tiles, finish, 0, unroll=4)


def apply_kernel(list_ref, count_ref, joined_ref, own_ref, diag_charge_ref, diag_potential_ref, link_ref,
                 store_ref, image_ref, vec_ref, sum_ref, ring_ref, sems):
    tiles = link_ref.shape[0]
    rows_all = vec_ref.shape[0]
    count = count_ref[0]
    turns = (count + APPLY_CHUNK - 1) // APPLY_CHUNK

    def in_copy(turn, first=0, places=APPLY_CHUNK):
        slot = lax.rem(turn, APPLY_RING)
        return pltpu.make_async_copy(
            store_ref.at[pl.ds(turn * APPLY_CHUNK + first, places)],
            ring_ref.at[slot, pl.ds(first, places)], sems.at[slot])

    def start_copies(turn):
        for first in range(0, APPLY_CHUNK, APPLY_COPY):
            in_copy(turn, first, APPLY_COPY).start()

    for turn in range(APPLY_RING - 1):
        @pl.when(turn < turns)
        def _():
            start_copies(turn)

    fill_vectors(joined_ref, 0, rows_all, vec_ref)

    def clear(tile, carry):
        sum_ref[tile] = jnp.zeros(sum_ref.shape[1:], jnp.float32)
        return carry

    lax.fori_loop(0, tiles + 1, clear, 0, unroll=4)

    def visit(turn, carry):
        slot = lax.rem(turn, APPLY_RING)

        @pl.when(turn + APPLY_RING - 1 < turns)
        def _():
            start_copies(turn + APPLY_RING - 1)

        in_copy(turn).wait()
        entries = [list_ref[turn * APPLY_CHUNK + place] for place in range(APPLY_CHUNK)]
        products = [
            block_product(vec_ref[(entry >> 14) & 255], ring_ref[slot, place])
            for place, entry in enumerate(entries)
        ]
        for entry, product in zip(entries, products):
            tile = entry & 255
            sum_ref[tile] = sum_ref[tile] + product
        return carry

    lax.fori_loop(0, turns, visit, 0)

    def finish(tile, carry):
        total = sum_ref[tile]
        one = pl.ds(tile, 1)
        values = own_ref[pl.ds(tile, 4, stride=tiles), :]
        pair_charge, pair_potential = pair_parts(total)
        image_ref[pl.ds(tile, 4, stride=tiles), :] = image_rows(
            values, pair_charge, pair_potential, diag_charge_ref[one, :], diag_potential_ref[one, :],
            link_ref[one, :])
        return carry

    lax.fori_loop(0, tiles, finish, 0, unroll=4)


def moment_kernel(zero_ref, one_ref, two_ref, three_ref, out_ref):
    tiles = zero_ref.shape[0] // 4
    refs = (zero_ref, one_ref, two_ref, three_ref)
    lane = lax.broadcasted_iota(jnp.int32, (1, 128), 1)
    for system in range(2):
        line = jnp.zeros((1, 128), jnp.float32)
        for degree in range(2 * ITERS):
            left, right = refs[degree // 2], refs[degree - degree // 2]
            low = slice(system * tiles, system * tiles + tiles)
            high = slice((2 + system) * tiles, (2 + system) * tiles + tiles)
            product = left[low, :] * right[low, :] + left[high, :] * right[high, :]
            line = jnp.where(lane == degree, jnp.sum(product, keepdims=True), line)
        out_ref[system : system + 1, :] = line


def combine_kernel(moments_ref, zero_ref, one_ref, two_ref, three_ref, solution_ref, residual_ref):
    tiles = zero_ref.shape[0] // 4
    total = jnp.sum(moments_ref[...], axis=0)
    moments = [total[:, degree : degree + 1] for degree in range(2 * ITERS)]

    def times(poly):
        grown = [SHIFT * c for c in poly] + [jnp.zeros_like(poly[0])]
        return [c + p for c, p in zip(grown, [jnp.zeros_like(poly[0])] + poly)]

    def product(left, right):
        out = 0.0
        for i, a in enumerate(left):
            for j, c in enumerate(right):
                out = out + a * c * moments[i + j]
        return out

    def axpy(left, scale, right):
        length = max(len(left), len(right))
        zero = jnp.zeros_like(scale)
        left = left + [zero] * (length - len(left))
        right = right + [zero] * (length - len(right))
        return [a + scale * c for a, c in zip(left, right)]

    one = jnp.ones_like(moments[0])
    found = [jnp.zeros_like(one)]
    rest = [one]
    direction = [one]
    norm = moments[0]
    for iteration in range(ITERS):
        along = times(direction)
        step = norm / product(direction, along)
        found = axpy(found, step, direction)
        rest = axpy(rest, -step, along)
        if iteration + 1 < ITERS:
            norm_next = product(rest, rest)
            direction = axpy(rest, norm_next / norm, direction)
            norm = norm_next
    refs = (zero_ref, one_ref, two_ref, three_ref)
    for field in range(4):
        system = field % 2
        span = slice(field * tiles, field * tiles + tiles)
        for poly, out_ref in ((found, solution_ref), (rest, residual_ref)):
            value = 0.0
            for c, ref in zip(poly, refs):
                value = value + c[system : system + 1, :] * ref[span, :]
            out_ref[span, :] = value


VMEM = pltpu.MemorySpace.VMEM
SMEM = pltpu.MemorySpace.SMEM


def in_vmem():
    return pl.BlockSpec(memory_space=VMEM)


def in_smem():
    return pl.BlockSpec(memory_space=SMEM)


def on_device(positions, shield, width, hardness, softness, coupling, pair_bits, right_side):
    extent = hardness.shape[:3]
    size = hardness.shape[3]
    tiles = extent[0] * extent[1] * extent[2]
    counts = {axis: lax.axis_size(axis) for axis in AXES}
    f32 = jnp.float32

    hard, soft, link = (a.reshape(tiles, size) for a in (hardness, softness, coupling))
    start = right_side.reshape(4, tiles, size)
    fields = jnp.concatenate(
        [positions.reshape(3, tiles, size), shield.reshape(1, tiles, size), width.reshape(1, tiles, size), start],
        axis=0)
    joined, boxes = extended(fields, extent)
    rows_all = joined.shape[1]
    table = candidate_table(boxes, extent, counts)
    capacity = table.shape[0] + max(2 * BUILD_SLOTS, APPLY_CHUNK)

    slots, count = pl.pallas_call(
        list_kernel,
        out_shape=(jax.ShapeDtypeStruct((capacity,), jnp.int32), jax.ShapeDtypeStruct((1,), jnp.int32)),
        in_specs=[in_smem(), in_smem()],
        out_specs=(in_smem(), in_smem()),
        name="pair_list",
    )(pair_bits.reshape(tiles), jnp.asarray(table))

    flat = (4 * tiles, size)
    start_flat = start.reshape(flat)
    store, diag_charge, diag_potential, image = pl.pallas_call(
        build_kernel,
        out_shape=(
            jax.ShapeDtypeStruct((capacity, 2 * size, size), jnp.bfloat16),
            jax.ShapeDtypeStruct((tiles, size), f32),
            jax.ShapeDtypeStruct((tiles, size), f32),
            jax.ShapeDtypeStruct(flat, f32),
        ),
        in_specs=[in_smem(), in_smem()] + [in_vmem()] * 5,
        out_specs=(pl.BlockSpec(memory_space=pl.ANY), in_vmem(), in_vmem(), in_vmem()),
        scratch_shapes=[
            pltpu.VMEM((rows_all, 8, size), f32),
            pltpu.VMEM((tiles, size, 5 * size), f32),
            pltpu.VMEM((rows_all, 16, size), jnp.bfloat16),
            pltpu.VMEM((tiles + 1, 16, 2 * size), f32),
            pltpu.VMEM((BUILD_RING, BUILD_SLOTS, 2 * size, size), jnp.bfloat16),
            pltpu.VMEM((BUILD_RING, BUILD_SLOTS, 2 * size, size), jnp.bfloat16),
            pltpu.SemaphoreType.DMA((2, BUILD_RING)),
        ],
        compiler_params=pltpu.CompilerParams(vmem_limit_bytes=40 * 2**20),
        name="build",
    )(slots, count, joined.reshape(-1, size), start_flat, hard, soft, link)

    def operate(vector):
        spread, _ = extended(vector.reshape(4, tiles, size), extent)
        return pl.pallas_call(
            apply_kernel,
            out_shape=jax.ShapeDtypeStruct(flat, f32),
            in_specs=[in_smem(), in_smem()] + [in_vmem()] * 5 + [pl.BlockSpec(memory_space=pl.ANY)],
            out_specs=in_vmem(),
            scratch_shapes=[
                pltpu.VMEM((rows_all, 16, size), jnp.bfloat16),
                pltpu.VMEM((tiles + 1, 16, 2 * size), f32),
                pltpu.VMEM((APPLY_RING, APPLY_CHUNK, 2 * size, size), jnp.bfloat16),
                pltpu.SemaphoreType.DMA((APPLY_RING,)),
            ],
            compiler_params=pltpu.CompilerParams(vmem_limit_bytes=40 * 2**20),
            name="apply",
        )(slots, count, spread.reshape(-1, size), vector, diag_charge, diag_potential, link, store)

    vectors = [start_flat, image]
    for _ in range(ITERS - 1):
        vectors.append(operate(vectors[-1]))

    moments = pl.pallas_call(
        moment_kernel,
        out_shape=jax.ShapeDtypeStruct((2, size), f32),
        in_specs=[in_vmem()] * 4,
        out_specs=in_vmem(),
        name="moments",
    )(*vectors)
    devices = counts["gx"] * counts["gy"] * counts["gz"]
    gathered = lax.all_to_all(jnp.broadcast_to(moments, (devices,) + moments.shape), AXES, 0, 0)
    solution, residual = pl.pallas_call(
        combine_kernel,
        out_shape=(jax.ShapeDtypeStruct(flat, f32), jax.ShapeDtypeStruct(flat, f32)),
        in_specs=[in_vmem()] * 5,
        out_specs=(in_vmem(), in_vmem()),
        name="combine",
    )(gathered, *vectors)
    return (solution.reshape(right_side.shape), residual.reshape(right_side.shape))


def solution(mesh):
    return jax.shard_map(
        on_device,
        mesh=mesh,
        in_specs=(
            P(None, "gx", "gy", "gz", None),
            P("gx", "gy", "gz", None),
            P("gx", "gy", "gz", None),
            P("gx", "gy", "gz", None),
            P("gx", "gy", "gz", None),
            P("gx", "gy", "gz", None),
            P("gx", "gy", "gz"),
            P(None, "gx", "gy", "gz", None),
        ),
        out_specs=(P(None, "gx", "gy", "gz", None), P(None, "gx", "gy", "gz", None)),
        check_vma=False,
    )
```

```python
import functools
import math

import jax
import jax.numpy as jnp
import numpy as np
from jax import lax
from jax.experimental import pallas as pl
from jax.experimental.pallas import tpu as pltpu
from jax.sharding import PartitionSpec as P

ITERS = 3

coulomb_scale = 0.002
response_scale = 0.003
length_scale = 1.0 / coulomb_scale
width_scale = -math.log(2.0) * length_scale * length_scale

SHIFT = 3.0

AXES = ("gx", "gy", "gz")
HALO_ORDER = (("gy", 1), ("gx", 0), ("gz", 2))
PARTS = 3
TURN_BITS = 3
TURN = 1 << TURN_BITS
BUILD_SLOTS = TURN // 2
BUILD_PAIRS = BUILD_SLOTS // 2
BUILD_RING = 8
APPLY_COPY = 1
APPLY_RING = 10


class Piece:
    def __init__(self, array, boxes):
        self.array = array
        self.boxes = boxes

    def face(self, dim, level):
        rows, boxes = [], []
        offset = 0
        for origin, shape in self.boxes:
            volume = shape[0] * shape[1] * shape[2]
            if origin[dim] <= level < origin[dim] + shape[dim]:
                part = self.array[:, offset : offset + volume]
                part = part.reshape((part.shape[0],) + shape + part.shape[2:])
                part = lax.slice_in_dim(part, level - origin[dim], level - origin[dim] + 1, axis=dim + 1)
                cut = tuple(1 if d == dim else shape[d] for d in range(3))
                rows.append(part.reshape(part.shape[0], -1, part.shape[-1]))
                boxes.append((tuple(level if d == dim else origin[d] for d in range(3)), cut))
            offset += volume
        return rows, boxes


def whole_face(pieces, dim, level):
    rows, boxes = [], []
    for piece in pieces:
        more_rows, more_boxes = piece.face(dim, level)
        rows += more_rows
        boxes += more_boxes
    return (jnp.concatenate(rows, axis=1) if len(rows) > 1 else rows[0]), boxes


def moved(boxes, dim, level):
    return [(tuple(level if d == dim else o[d] for d in range(3)), s) for o, s in boxes]


def extended(block, extent):
    pieces = [Piece(block, [((0, 0, 0), extent)])]
    for axis, dim in HALO_ORDER:
        count = lax.axis_size(axis)
        if count == 1:
            continue
        size = extent[dim]
        first, boxes = whole_face(pieces, dim, 0)
        last, _ = whole_face(pieces, dim, size - 1)
        if count == 2:
            sent = jnp.where(lax.axis_index(axis) == 0, last, first)
            got = lax.ppermute(sent, axis, [(0, 1), (1, 0)])
            pieces = pieces + [Piece(got, moved(boxes, dim, size))]
        else:
            forward = [(i, (i + 1) % count) for i in range(count)]
            backward = [(target, source) for source, target in forward]
            low = lax.ppermute(last, axis, forward)
            high = lax.ppermute(first, axis, backward)
            pieces = pieces + [
                Piece(low, moved(boxes, dim, -1)),
                Piece(high, moved(boxes, dim, size)),
            ]
    joined = jnp.concatenate([piece.array for piece in pieces], axis=1)
    return joined, [box for piece in pieces for box in piece.boxes]


def storage_rows(boxes, extent, counts):
    rows = {}
    offset = 0
    for origin, shape in boxes:
        for a in range(shape[0]):
            for b in range(shape[1]):
                for c in range(shape[2]):
                    rows[(origin[0] + a, origin[1] + b, origin[2] + c)] = offset
                    offset += 1

    def row_of(coord):
        fixed = list(coord)
        for axis, dim in HALO_ORDER:
            outside = not 0 <= fixed[dim] < extent[dim]
            if outside and counts[axis] == 1:
                fixed[dim] = 0
            elif outside and counts[axis] == 2:
                fixed[dim] = extent[dim]
        return rows[tuple(fixed)]

    return row_of


def candidate_pairs(boxes, extent, counts):
    row_of = storage_rows(boxes, extent, counts)
    tiles = extent[0] * extent[1] * extent[2]
    halo, inner = [], []
    for x in range(extent[0]):
        for y in range(extent[1]):
            for z in range(extent[2]):
                own = (x * extent[1] + y) * extent[2] + z
                halo.append([])
                inner.append([])
                for code in range(27):
                    a, b, c = code // 9, code // 3 % 3, code % 3
                    partner = row_of((x + a - 1, y + b - 1, z + c - 1))
                    assert own < 255 and partner < 255
                    entry = packed(own, partner, a, b, c)
                    if partner >= tiles:
                        halo[-1].append((code, entry))
                    elif partner > own:
                        inner[-1].append((code, entry))
    return halo, inner


def packed(own, partner, a=1, b=1, c=1):
    return own | a << 8 | b << 10 | c << 12 | partner << 14


def own_of(entry):
    return entry & 255


def partner_of(entry):
    return (entry >> 14) & 255


def list_table(found_of, never):
    longest = max(len(found) for found in found_of)
    table = [
        [entry | code << 22 for code, entry in found] + [never | 31 << 22] * (longest - len(found))
        for found in found_of
    ]
    return np.asarray([entry - (1 << 32) if entry >> 31 else entry for row in table for entry in row], np.int32)


def list_kernel(bits_ref, halo_ref, inner_ref, list_ref, word_ref, *, spare):
    height, depth = bits_ref.shape[1:]
    tiles = word_ref.shape[0]
    for tile in range(tiles):
        list_ref[tile] = jnp.int32(packed(tile, tile))
        word_ref[tile] = bits_ref[tile // (height * depth), tile // depth % height, tile % depth]
    filled = jnp.int32(tiles)
    for part, table_ref in enumerate((halo_ref, inner_ref)):
        longest = table_ref.shape[0] // tiles

        def visit(tile, filled):
            word = word_ref[tile]
            for place in range(longest):
                entry = table_ref[tile * longest + place]
                list_ref[filled] = entry
                filled = filled + ((word >> ((entry >> 22) & 31)) & 1)
            list_ref[filled] = tile | packed(0, spare)
            return filled + (filled & 1)

        filled = lax.fori_loop(0, tiles, visit, filled)

        def pad(extra, carry):
            list_ref[filled + extra] = jnp.int32(packed(tiles, spare))
            return carry

        lax.fori_loop(0, TURN, pad, 0)
        filled = (filled + TURN - 1) & -TURN
        list_ref[list_ref.shape[0] - 2 + part] = filled >> TURN_BITS


def split_rows(values):
    parts = []
    rest = values
    for _ in range(PARTS):
        part = rest.astype(jnp.bfloat16).astype(jnp.float32)
        parts.append(part)
        rest = rest - part
    return parts


def fill_vectors(source_ref, first_row, rows_all, vec_ref):
    vec_ref[rows_all] = jnp.zeros(vec_ref.shape[1:], jnp.bfloat16)

    def one(tile, carry):
        values = source_ref[pl.ds(first_row + tile, 4, stride=rows_all), :]
        parts = split_rows(values)
        stacked = jnp.concatenate(parts + [jnp.ones_like(values)], axis=0)
        vec_ref[tile] = stacked.astype(jnp.bfloat16)
        return carry

    lax.fori_loop(0, rows_all, one, 0, unroll=8)


def pair_parts(total):
    joined = total[0:4] + total[4:8] + total[8:12]
    return joined[0:2, 0:128], joined[2:4, 128:256]


def image_rows(values, pair_charge, pair_potential, diag_charge, diag_potential, linking):
    charge, potential = values[0:2], values[2:4]
    image_charge = diag_charge * charge + pair_charge + linking * potential
    image_potential = diag_potential * potential - pair_potential + linking * charge
    return jnp.concatenate([image_charge, image_potential], axis=0)


def add_products(vec_ref, sum_ref, blocks, entries, kind):
    spare_sum = sum_ref.shape[0] - 1
    added = []

    def times(vectors, block):
        return jnp.dot(vectors, block, preferred_element_type=jnp.float32)

    for place, block in enumerate(blocks):
        pair = entries[2 * place : 2 * place + 2]
        half = block().shape[0] // 2
        if kind == "own":
            for side, entry in enumerate(pair):
                vectors = vec_ref[own_of(entry)]
                lanes = slice(side * half, side * half + half)
                added.append((own_of(entry), lax.dot_general(
                    vectors, block()[:, lanes], (((1,), (1,)), ((), ())), preferred_element_type=jnp.float32)))
            continue
        vectors = jnp.concatenate([vec_ref[partner_of(entry)] for entry in pair], axis=1)
        added.append((own_of(pair[0]), lax.dot_general(
            vectors, block(), (((1,), (1,)), ((), ())), preferred_element_type=jnp.float32)))
        if kind == "inner":
            vectors = vec_ref[own_of(pair[0])]
            coulomb, response = times(vectors, block()[:half]), times(vectors, block()[half:])
            for side, entry in enumerate(pair):
                lanes = slice(side * half, side * half + half)
                added.append((
                    jnp.minimum(partner_of(entry), spare_sum),
                    jnp.concatenate([coulomb[:, lanes], response[:, lanes]], axis=1)))
    for tile, product in added:
        sum_ref[tile] = sum_ref[tile] + product


def build_kernel(list_hbm, joined_ref, hard_hbm, soft_hbm, link_hbm,
                 store_ref, diag_ref, image_ref,
                 row_ref, spread_ref, vec_ref, sum_ref, even_ref, odd_ref,
                 local_ref, list_ref, apart_ref, sems, local_sems):
    tiles, size = hard_hbm.shape
    rows_all = vec_ref.shape[0] - 1

    def local_copies():
        return [
            pltpu.make_async_copy(source, local_ref.at[place], local_sems.at[place])
            for place, source in enumerate((hard_hbm, soft_hbm, link_hbm))
        ]

    list_copy = pltpu.make_async_copy(list_hbm, list_ref, local_sems.at[3])
    list_copy.start()
    for copy in local_copies():
        copy.start()

    field = lax.broadcasted_iota(jnp.int32, (8, size), 0)
    scale = jnp.where(field < 4, jnp.float32(length_scale), jnp.float32(width_scale))

    def prepare(tile, carry):
        row_ref[tile] = joined_ref[pl.ds(tile, 8, stride=rows_all), :] * scale
        return carry

    lax.fori_loop(0, rows_all, prepare, 0, unroll=8)
    row_ref[rows_all] = jnp.ones((8, size), jnp.float32)
    fill_vectors(joined_ref, 5 * rows_all, rows_all, vec_ref)

    atom = lax.broadcasted_iota(jnp.int32, (size, size), 0)
    partner_atom = lax.broadcasted_iota(jnp.int32, (size, size), 1)
    apart_ref[...] = jnp.where(atom == partner_atom, jnp.inf, 0.0).astype(jnp.float32)

    line = lax.broadcasted_iota(jnp.int32, (32, 5 * size), 0)
    chosen = lax.broadcasted_iota(jnp.int32, (32, 5 * size), 1) // size
    select = jnp.where(((line & 7) == chosen) & (line < 24), 1.0, 0.0).astype(jnp.bfloat16)

    def spread(tile, carry):
        params = row_ref[tile]
        stacked = jnp.concatenate(split_rows(params) + [jnp.zeros_like(params)], axis=0)
        spread_ref[tile] = lax.dot_general(
            stacked.astype(jnp.bfloat16), select, (((0,), (0,)), ((), ())), preferred_element_type=jnp.float32)
        sum_ref[tile] = jnp.zeros(sum_ref.shape[1:], jnp.float32)
        return carry

    lax.fori_loop(0, tiles, spread, 0, unroll=2)
    sum_ref[tiles] = jnp.zeros(sum_ref.shape[1:], jnp.float32)

    def multiply(ring_ref, base, entries, kind):
        blocks = [lambda place=place: ring_ref[base, place] for place in range(BUILD_PAIRS)]
        add_products(vec_ref, sum_ref, blocks, entries, kind)

    def out_copy(ring_ref, half, base, first):
        return pltpu.make_async_copy(
            ring_ref.at[base], store_ref.at[pl.ds(first, BUILD_PAIRS)], sems.at[half, base])

    def pair_block(ring_ref, base, slot, entry, own_pairs):
        own = jnp.minimum(own_of(entry), tiles - 1)
        partner = partner_of(entry)
        place, lanes = slot // 2, slice(slot % 2 * size, slot % 2 * size + size)
        shift_a = (((entry >> 8) & 3) - 1).astype(jnp.float32) * length_scale
        shift_b = (((entry >> 10) & 3) - 1).astype(jnp.float32) * length_scale
        shift_c = (((entry >> 12) & 3) - 1).astype(jnp.float32) * length_scale
        theirs = row_ref[partner]
        full = (16, size)
        their_a = jnp.broadcast_to(theirs[0:1] + shift_a, full)
        their_b = jnp.broadcast_to(theirs[1:2] + shift_b, full)
        their_c = jnp.broadcast_to(theirs[2:3] + shift_c, full)
        their_shield = jnp.broadcast_to(theirs[3:4], full)
        their_width = jnp.broadcast_to(theirs[4:5], full)
        for group in range(size // 16):
            rows = slice(16 * group, 16 * group + 16)

            def mine(c):
                return spread_ref[own, rows, c * size : (c + 1) * size]

            delta_a = their_a - mine(0)
            delta_b = their_b - mine(1)
            delta_c = their_c - mine(2)
            distance = delta_a * delta_a + delta_b * delta_b + delta_c * delta_c
            if own_pairs:
                distance = distance + apart_ref[rows, :]
            coulomb = lax.rsqrt(distance + mine(3) * their_shield)
            response = response_scale * jnp.exp2(distance / (mine(4) + their_width))
            ring_ref[base, place, rows, lanes] = coulomb.astype(jnp.bfloat16)
            ring_ref[base, place, size + 16 * group : size + 16 * group + 16, lanes] = response.astype(jnp.bfloat16)

    def entries_at(first):
        return [list_ref[first + slot] for slot in range(BUILD_SLOTS)]

    def turns(first, last, kind):
        def visit(turn, carry):
            base = lax.rem(turn, BUILD_RING)
            before = lax.rem(turn + BUILD_RING - 1, BUILD_RING)
            start = turn * TURN

            @pl.when(turn >= BUILD_RING)
            def _():
                out_copy(even_ref, 0, base, 0).wait()
                out_copy(odd_ref, 1, base, 0).wait()

            late = [
                jnp.where(turn > first, list_ref[jnp.maximum(start - BUILD_SLOTS + slot, 0)], nothing)
                for slot in range(BUILD_SLOTS)
            ]
            even, odd = entries_at(start), entries_at(start + BUILD_SLOTS)
            multiply(odd_ref, before, late, kind)
            for slot, entry in enumerate(even):
                pair_block(even_ref, base, slot, entry, kind == "own")
            multiply(even_ref, base, even, kind)
            for slot, entry in enumerate(odd):
                pair_block(odd_ref, base, slot, entry, kind == "own")
            out_copy(even_ref, 0, base, 2 * BUILD_PAIRS * turn).start()
            out_copy(odd_ref, 1, base, 2 * BUILD_PAIRS * turn + BUILD_PAIRS).start()
            return carry

        lax.fori_loop(first, last, visit, 0)

        @pl.when(last > first)
        def _():
            final = last - 1
            multiply(odd_ref, lax.rem(final, BUILD_RING), entries_at(final * TURN + BUILD_SLOTS), kind)

    nothing = packed(tiles, rows_all)
    assert tiles % TURN == 0
    own_turns = tiles // TURN
    list_copy.wait()
    halo_turns = list_ref[list_ref.shape[0] - 2]
    all_turns = list_ref[list_ref.shape[0] - 1]
    turns(0, jnp.minimum(halo_turns, own_turns), "own")
    turns(own_turns, halo_turns, "halo")
    turns(halo_turns, all_turns, "inner")
    for group in range(BUILD_RING):
        @pl.when(group < all_turns)
        def _():
            out_copy(even_ref, 0, group, 0).wait()
            out_copy(odd_ref, 1, group, 0).wait()

    for copy in local_copies():
        copy.wait()

    def finish(tile, carry):
        total = sum_ref[tile]
        one = pl.ds(tile, 1)
        diag_charge = local_ref[0, one, :] + total[12:13, 0:128] - SHIFT
        diag_potential = local_ref[1, one, :] + total[12:13, 128:256] - SHIFT
        linking = local_ref[2, one, :]
        diag_ref[0, one, :] = diag_charge
        diag_ref[1, one, :] = diag_potential
        diag_ref[2, one, :] = linking
        values = joined_ref[pl.ds(5 * rows_all + tile, 4, stride=rows_all), :]
        pair_charge, pair_potential = pair_parts(total)
        image_ref[pl.ds(tile, 4, stride=tiles), :] = image_rows(
            values, pair_charge, pair_potential, diag_charge, diag_potential, linking)
        return carry

    lax.fori_loop(0, tiles, finish, 0, unroll=4)


def apply_kernel(*refs):
    list_hbm, joined_ref, diag_hbm, store_ref = refs[:4]
    last = len(refs) > 12
    earlier_hbm = refs[4:6] if last else ()
    image_ref = refs[4 + len(earlier_hbm)]
    moment_ref = refs[7] if last else None
    vec_ref, sum_ref, ring_ref, diag_ref, list_ref = refs[8:13] if last else refs[5:10]
    earlier_refs = refs[13:15] if last else ()
    sems, local_sems = refs[-2:]

    tiles = diag_hbm.shape[1]
    rows_all = vec_ref.shape[0] - 1
    own_turns = tiles // TURN

    def in_copy(turn, first=0, places=TURN // 2):
        slot = lax.rem(turn, APPLY_RING)
        return pltpu.make_async_copy(
            store_ref.at[pl.ds(turn * (TURN // 2) + first, places)],
            ring_ref.at[slot, pl.ds(first, places)], sems.at[slot])

    def start_copies(turn):
        for first in range(0, TURN // 2, APPLY_COPY):
            in_copy(turn, first, APPLY_COPY).start()

    def local_copies():
        pairs = [(diag_hbm, diag_ref)] + list(zip(earlier_hbm, earlier_refs))
        return [
            pltpu.make_async_copy(source, target, local_sems.at[place])
            for place, (source, target) in enumerate(pairs)
        ]

    ahead = APPLY_RING - 1
    list_copy = pltpu.make_async_copy(list_hbm, list_ref, local_sems.at[len(earlier_hbm) + 1])
    list_copy.start()
    for turn in range(min(ahead, own_turns)):
        start_copies(jnp.int32(turn))
    for copy in local_copies():
        copy.start()

    fill_vectors(joined_ref, 0, rows_all, vec_ref)

    def clear(tile, carry):
        sum_ref[tile] = jnp.zeros(sum_ref.shape[1:], jnp.float32)
        return carry

    lax.fori_loop(0, tiles + 1, clear, 0, unroll=4)

    list_copy.wait()
    halo_turns = list_ref[list_ref.shape[0] - 2]
    all_turns = list_ref[list_ref.shape[0] - 1]
    for turn in range(own_turns, ahead):
        @pl.when(turn < all_turns)
        def _():
            start_copies(jnp.int32(turn))

    def visits(first, last, kind):
        def visit(turn, carry):
            slot = lax.rem(turn, APPLY_RING)

            @pl.when(turn + ahead < all_turns)
            def _():
                start_copies(turn + ahead)

            in_copy(turn).wait()
            entries = [list_ref[turn * TURN + place] for place in range(TURN)]
            blocks = [lambda place=place: ring_ref[slot, place] for place in range(TURN // 2)]
            add_products(vec_ref, sum_ref, blocks, entries, kind)
            return carry

        lax.fori_loop(first, last, visit, 0)

    visits(0, own_turns, "own")
    visits(own_turns, halo_turns, "halo")
    visits(halo_turns, all_turns, "inner")
    for copy in local_copies():
        copy.wait()

    def finish(tile, carry):
        total = sum_ref[tile]
        one = pl.ds(tile, 1)
        values = joined_ref[pl.ds(tile, 4, stride=rows_all), :]
        pair_charge, pair_potential = pair_parts(total)
        image_ref[pl.ds(tile, 4, stride=tiles), :] = image_rows(
            values, pair_charge, pair_potential, diag_ref[0, one, :], diag_ref[1, one, :], diag_ref[2, one, :])
        return carry

    lax.fori_loop(0, tiles, finish, 0, unroll=4)

    if last:
        lane = lax.broadcasted_iota(jnp.int32, (1, 128), 1)

        def rows_of(order, field):
            if order == 2:
                return joined_ref[field * rows_all : field * rows_all + tiles, :]
            ref = (earlier_refs[0], earlier_refs[1], None, image_ref)[order]
            return ref[field * tiles : (field + 1) * tiles, :]

        lines = []
        for system in range(2):
            line = jnp.zeros((1, 128), jnp.float32)
            for degree in range(2 * ITERS):
                left, right = degree // 2, degree - degree // 2
                product = rows_of(left, system) * rows_of(right, system)
                product = product + rows_of(left, 2 + system) * rows_of(right, 2 + system)
                line = jnp.where(lane == degree, jnp.sum(product, keepdims=True), line)
            lines.append(line)
        both = jnp.concatenate(lines, axis=0)
        moment_ref[...] = jnp.broadcast_to(both[None], moment_ref.shape)


def combine_kernel(moments_ref, zero_ref, one_ref, two_ref, three_ref, solution_ref, residual_ref):
    tiles = zero_ref.shape[0] // 4
    total = jnp.sum(moments_ref[...], axis=0)
    moments = [total[:, degree : degree + 1] for degree in range(2 * ITERS)]

    def times(poly):
        grown = [SHIFT * c for c in poly] + [jnp.zeros_like(poly[0])]
        return [c + p for c, p in zip(grown, [jnp.zeros_like(poly[0])] + poly)]

    def product(left, right):
        out = 0.0
        for i, a in enumerate(left):
            for j, c in enumerate(right):
                out = out + a * c * moments[i + j]
        return out

    def axpy(left, scale, right):
        length = max(len(left), len(right))
        zero = jnp.zeros_like(scale)
        left = left + [zero] * (length - len(left))
        right = right + [zero] * (length - len(right))
        return [a + scale * c for a, c in zip(left, right)]

    one = jnp.ones_like(moments[0])
    found = [jnp.zeros_like(one)]
    rest = [one]
    direction = [one]
    norm = moments[0]
    for iteration in range(ITERS):
        along = times(direction)
        step = norm / product(direction, along)
        found = axpy(found, step, direction)
        rest = axpy(rest, -step, along)
        if iteration + 1 < ITERS:
            norm_next = product(rest, rest)
            direction = axpy(rest, norm_next / norm, direction)
            norm = norm_next
    refs = (zero_ref, one_ref, two_ref, three_ref)
    for field in range(4):
        system = field % 2
        span = slice(field * tiles, field * tiles + tiles)
        for poly, out_ref in ((found, solution_ref), (rest, residual_ref)):
            value = 0.0
            for c, ref in zip(poly, refs):
                value = value + c[system : system + 1, :] * ref[span, :]
            out_ref[span, :] = value


VMEM = pltpu.MemorySpace.VMEM
SMEM = pltpu.MemorySpace.SMEM


def in_vmem():
    return pl.BlockSpec(memory_space=VMEM)


def in_hbm():
    return pl.BlockSpec(memory_space=pltpu.MemorySpace.HBM)


def pinned(array):
    return pltpu.with_memory_space_constraint(array, pltpu.MemorySpace.HBM)


def in_smem():
    return pl.BlockSpec(memory_space=SMEM)


def on_device(positions, shield, width, hardness, softness, coupling, pair_bits, right_side):
    extent = hardness.shape[:3]
    size = hardness.shape[3]
    tiles = extent[0] * extent[1] * extent[2]
    counts = {axis: lax.axis_size(axis) for axis in AXES}
    f32 = jnp.float32

    hard, soft, link = (a.reshape(tiles, size) for a in (hardness, softness, coupling))
    start = right_side.reshape(4, tiles, size)
    fields = jnp.concatenate(
        [positions.reshape(3, tiles, size), shield.reshape(1, tiles, size), width.reshape(1, tiles, size), start],
        axis=0)
    joined, boxes = extended(fields, extent)
    rows_all = joined.shape[1]
    halo, inner = candidate_pairs(boxes, extent, counts)
    entries = tiles + sum(-(-len(found) // 2) * 2 for found in halo + inner)
    entries = -(-(entries + 3 * TURN) // TURN) * TURN

    tables = [jnp.asarray(list_table(found, packed(tiles, rows_all))) for found in (halo, inner)]
    slots = pl.pallas_call(
        functools.partial(list_kernel, spare=rows_all),
        out_shape=jax.ShapeDtypeStruct((entries + 2,), jnp.int32),
        in_specs=[in_smem()] * 3,
        out_specs=in_smem(),
        scratch_shapes=[pltpu.SMEM((tiles,), jnp.int32)],
        name="pair_list",
    )(pair_bits, *tables)
    slots = pinned(slots)

    flat = (4 * tiles, size)
    start_flat = start.reshape(flat)
    store, diag, image = pl.pallas_call(
        build_kernel,
        out_shape=(
            jax.ShapeDtypeStruct((entries // 2, 2 * size, 2 * size), jnp.bfloat16),
            jax.ShapeDtypeStruct((3, tiles, size), f32),
            jax.ShapeDtypeStruct(flat, f32),
        ),
        in_specs=[in_hbm(), in_vmem()] + [in_hbm()] * 3,
        out_specs=(in_hbm(), in_vmem(), in_vmem()),
        scratch_shapes=[
            pltpu.VMEM((rows_all + 1, 8, size), f32),
            pltpu.VMEM((tiles, size, 5 * size), f32),
            pltpu.VMEM((rows_all + 1, 16, size), jnp.bfloat16),
            pltpu.VMEM((tiles + 1, 16, 2 * size), f32),
            pltpu.VMEM((BUILD_RING, BUILD_PAIRS, 2 * size, 2 * size), jnp.bfloat16),
            pltpu.VMEM((BUILD_RING, BUILD_PAIRS, 2 * size, 2 * size), jnp.bfloat16),
            pltpu.VMEM((3, tiles, size), f32),
            pltpu.SMEM((entries + 2,), jnp.int32),
            pltpu.VMEM((size, size), f32),
            pltpu.SemaphoreType.DMA((2, BUILD_RING)),
            pltpu.SemaphoreType.DMA((4,)),
        ],
        compiler_params=pltpu.CompilerParams(vmem_limit_bytes=40 * 2**20),
        name="build",
    )(slots, joined.reshape(-1, size), pinned(hard), pinned(soft), pinned(link))

    devices = counts["gx"] * counts["gy"] * counts["gz"]
    diag = pinned(diag)

    def operate(vector, earlier=()):
        spread, _ = extended(vector.reshape(4, tiles, size), extent)
        last = len(earlier) > 0
        more = len(earlier)
        image_shape = jax.ShapeDtypeStruct(flat, f32)
        moment_shape = jax.ShapeDtypeStruct((devices, 2, size), f32)
        return pl.pallas_call(
            apply_kernel,
            out_shape=(image_shape, moment_shape) if last else image_shape,
            in_specs=[in_hbm(), in_vmem()] + [in_hbm()] * (2 + more),
            out_specs=(in_vmem(), in_vmem()) if last else in_vmem(),
            scratch_shapes=[
                pltpu.VMEM((rows_all + 1, 16, size), jnp.bfloat16),
                pltpu.VMEM((tiles + 1, 16, 2 * size), f32),
                pltpu.VMEM((APPLY_RING, TURN // 2, 2 * size, 2 * size), jnp.bfloat16),
                pltpu.VMEM((3, tiles, size), f32),
                pltpu.SMEM((entries + 2,), jnp.int32),
            ] + [pltpu.VMEM(flat, f32)] * more + [
                pltpu.SemaphoreType.DMA((APPLY_RING,)),
                pltpu.SemaphoreType.DMA((2 + more,)),
            ],
            compiler_params=pltpu.CompilerParams(vmem_limit_bytes=40 * 2**20),
            name="apply_last" if last else "apply",
        )(slots, spread.reshape(-1, size), diag, store, *[pinned(v) for v in earlier])

    second = operate(image)
    third, moments = operate(second, (start_flat, image))
    vectors = (start_flat, image, second, third)
    gathered = lax.all_to_all(moments, AXES, 0, 0)
    solution, residual = pl.pallas_call(
        combine_kernel,
        out_shape=(jax.ShapeDtypeStruct(flat, f32), jax.ShapeDtypeStruct(flat, f32)),
        in_specs=[in_vmem()] * 5,
        out_specs=(in_vmem(), in_vmem()),
        name="combine",
    )(gathered, *vectors)
    return (solution.reshape(right_side.shape), residual.reshape(right_side.shape))


def solution(mesh):
    return jax.shard_map(
        on_device,
        mesh=mesh,
        in_specs=(
            P(None, "gx", "gy", "gz", None),
            P("gx", "gy", "gz", None),
            P("gx", "gy", "gz", None),
            P("gx", "gy", "gz", None),
            P("gx", "gy", "gz", None),
            P("gx", "gy", "gz", None),
            P("gx", "gy", "gz"),
            P(None, "gx", "gy", "gz", None),
        ),
        out_specs=(P(None, "gx", "gy", "gz", None), P(None, "gx", "gy", "gz", None)),
        check_vma=False,
    )
```

```python
import functools
import math

import jax
import jax.numpy as jnp
import numpy as np
from jax import lax
from jax.experimental import pallas as pl
from jax.experimental.pallas import tpu as pltpu
from jax.sharding import PartitionSpec as P

ITERS = 3

coulomb_scale = 0.002
response_scale = 0.003
length_scale = 1.0 / coulomb_scale
width_scale = -math.log(2.0) * length_scale * length_scale

SHIFT = 3.0

AXES = ("gx", "gy", "gz")
HALO_ORDER = (("gy", 1), ("gx", 0), ("gz", 2))
PARTS = 3
TURN_BITS = 3
TURN = 1 << TURN_BITS
BUILD_SLOTS = TURN // 2
BUILD_PAIRS = BUILD_SLOTS // 2
BUILD_RING = 8
APPLY_COPY = 1
APPLY_RING = 12
APPLY_MERGE = 3


class Piece:
    def __init__(self, array, boxes):
        self.array = array
        self.boxes = boxes

    def face(self, dim, level):
        rows, boxes = [], []
        offset = 0
        for origin, shape in self.boxes:
            volume = shape[0] * shape[1] * shape[2]
            if origin[dim] <= level < origin[dim] + shape[dim]:
                part = self.array[:, offset : offset + volume]
                part = part.reshape((part.shape[0],) + shape + part.shape[2:])
                part = lax.slice_in_dim(part, level - origin[dim], level - origin[dim] + 1, axis=dim + 1)
                cut = tuple(1 if d == dim else shape[d] for d in range(3))
                rows.append(part.reshape(part.shape[0], -1, part.shape[-1]))
                boxes.append((tuple(level if d == dim else origin[d] for d in range(3)), cut))
            offset += volume
        return rows, boxes


def whole_face(pieces, dim, level):
    rows, boxes = [], []
    for piece in pieces:
        more_rows, more_boxes = piece.face(dim, level)
        rows += more_rows
        boxes += more_boxes
    return (jnp.concatenate(rows, axis=1) if len(rows) > 1 else rows[0]), boxes


def moved(boxes, dim, level):
    return [(tuple(level if d == dim else o[d] for d in range(3)), s) for o, s in boxes]


def extended(block, extent):
    pieces = [Piece(block, [((0, 0, 0), extent)])]
    for axis, dim in HALO_ORDER:
        count = lax.axis_size(axis)
        if count == 1:
            continue
        size = extent[dim]
        first, boxes = whole_face(pieces, dim, 0)
        last, _ = whole_face(pieces, dim, size - 1)
        if count == 2:
            sent = jnp.where(lax.axis_index(axis) == 0, last, first)
            got = lax.ppermute(sent, axis, [(0, 1), (1, 0)])
            pieces = pieces + [Piece(got, moved(boxes, dim, size))]
        else:
            forward = [(i, (i + 1) % count) for i in range(count)]
            backward = [(target, source) for source, target in forward]
            low = lax.ppermute(last, axis, forward)
            high = lax.ppermute(first, axis, backward)
            pieces = pieces + [
                Piece(low, moved(boxes, dim, -1)),
                Piece(high, moved(boxes, dim, size)),
            ]
    joined = jnp.concatenate([piece.array for piece in pieces], axis=1)
    return joined, [box for piece in pieces for box in piece.boxes]


def storage_rows(boxes, extent, counts):
    rows = {}
    offset = 0
    for origin, shape in boxes:
        for a in range(shape[0]):
            for b in range(shape[1]):
                for c in range(shape[2]):
                    rows[(origin[0] + a, origin[1] + b, origin[2] + c)] = offset
                    offset += 1

    def row_of(coord):
        fixed = list(coord)
        for axis, dim in HALO_ORDER:
            outside = not 0 <= fixed[dim] < extent[dim]
            if outside and counts[axis] == 1:
                fixed[dim] = 0
            elif outside and counts[axis] == 2:
                fixed[dim] = extent[dim]
        return rows[tuple(fixed)]

    return row_of


def candidate_pairs(boxes, extent, counts):
    row_of = storage_rows(boxes, extent, counts)
    tiles = extent[0] * extent[1] * extent[2]
    halo, inner = [], []
    for x in range(extent[0]):
        for y in range(extent[1]):
            for z in range(extent[2]):
                own = (x * extent[1] + y) * extent[2] + z
                halo.append([])
                inner.append([])
                for code in range(27):
                    a, b, c = code // 9, code // 3 % 3, code % 3
                    partner = row_of((x + a - 1, y + b - 1, z + c - 1))
                    assert own < 255 and partner < 255
                    entry = packed(own, partner, a, b, c)
                    if partner >= tiles:
                        halo[-1].append((code, entry))
                    elif partner > own:
                        inner[-1].append((code, entry))
    return halo, inner


def packed(own, partner, a=1, b=1, c=1):
    return own | a << 8 | b << 10 | c << 12 | partner << 14


def own_of(entry):
    return entry & 255


def partner_of(entry):
    return (entry >> 14) & 255


def list_table(found_of, never):
    longest = max(len(found) for found in found_of)
    table = [
        [entry | code << 22 for code, entry in found] + [never | 31 << 22] * (longest - len(found))
        for found in found_of
    ]
    return np.asarray([entry - (1 << 32) if entry >> 31 else entry for row in table for entry in row], np.int32)


def list_kernel(bits_ref, halo_ref, inner_ref, list_ref, word_ref, *, spare):
    height, depth = bits_ref.shape[1:]
    tiles = word_ref.shape[0]
    for tile in range(tiles):
        list_ref[tile] = jnp.int32(packed(tile, tile))
        word_ref[tile] = bits_ref[tile // (height * depth), tile // depth % height, tile % depth]
    filled = jnp.int32(tiles)
    for part, table_ref in enumerate((halo_ref, inner_ref)):
        longest = table_ref.shape[0] // tiles

        def visit(tile, filled):
            word = word_ref[tile]
            for place in range(longest):
                entry = table_ref[tile * longest + place]
                list_ref[filled] = entry
                filled = filled + ((word >> ((entry >> 22) & 31)) & 1)
            list_ref[filled] = tile | packed(0, spare)
            return filled + (filled & 1)

        filled = lax.fori_loop(0, tiles, visit, filled)

        def pad(extra, carry):
            list_ref[filled + extra] = jnp.int32(packed(tiles, spare))
            return carry

        lax.fori_loop(0, TURN, pad, 0)
        filled = (filled + TURN - 1) & -TURN
        list_ref[list_ref.shape[0] - 2 + part] = filled >> TURN_BITS


def split_rows(values):
    parts = []
    rest = values
    for _ in range(PARTS):
        part = rest.astype(jnp.bfloat16).astype(jnp.float32)
        parts.append(part)
        rest = rest - part
    return parts


def fill_vectors(source_ref, first_row, rows_all, vec_ref):
    vec_ref[rows_all] = jnp.zeros(vec_ref.shape[1:], jnp.bfloat16)

    def one(tile, carry):
        values = source_ref[pl.ds(first_row + tile, 4, stride=rows_all), :]
        parts = split_rows(values)
        stacked = jnp.concatenate(parts + [jnp.ones_like(values)], axis=0)
        vec_ref[tile] = stacked.astype(jnp.bfloat16)
        return carry

    lax.fori_loop(0, rows_all, one, 0, unroll=8)


def pair_parts(total):
    joined = total[0:4] + total[4:8] + total[8:12]
    return joined[0:2, 0:128], joined[2:4, 128:256]


def image_rows(values, pair_charge, pair_potential, diag_charge, diag_potential, linking):
    charge, potential = values[0:2], values[2:4]
    image_charge = diag_charge * charge + pair_charge + linking * potential
    image_potential = diag_potential * potential - pair_potential + linking * charge
    return jnp.concatenate([image_charge, image_potential], axis=0)


def add_products(vec_ref, sum_ref, blocks, entries, kind):
    spare_sum = sum_ref.shape[0] - 1
    added = []

    def times(vectors, block):
        return jnp.dot(vectors, block, preferred_element_type=jnp.float32)

    for place, block in enumerate(blocks):
        pair = entries[2 * place : 2 * place + 2]
        half = block().shape[0] // 2
        if kind == "own":
            for side, entry in enumerate(pair):
                vectors = vec_ref[own_of(entry)]
                lanes = slice(side * half, side * half + half)
                added.append((own_of(entry), lax.dot_general(
                    vectors, block()[:, lanes], (((1,), (1,)), ((), ())), preferred_element_type=jnp.float32)))
            continue
        vectors = jnp.concatenate([vec_ref[partner_of(entry)] for entry in pair], axis=1)
        added.append((own_of(pair[0]), lax.dot_general(
            vectors, block(), (((1,), (1,)), ((), ())), preferred_element_type=jnp.float32)))
        if kind == "inner":
            vectors = vec_ref[own_of(pair[0])]
            coulomb, response = times(vectors, block()[:half]), times(vectors, block()[half:])
            for side, entry in enumerate(pair):
                lanes = slice(side * half, side * half + half)
                added.append((
                    jnp.minimum(partner_of(entry), spare_sum),
                    jnp.concatenate([coulomb[:, lanes], response[:, lanes]], axis=1)))
    for tile, product in added:
        sum_ref[tile] = sum_ref[tile] + product


def build_kernel(list_hbm, joined_ref, hard_hbm, soft_hbm, link_hbm,
                 store_ref, diag_ref, image_ref,
                 row_ref, spread_ref, vec_ref, sum_ref, even_ref, odd_ref,
                 local_ref, list_ref, apart_ref, sems, local_sems):
    tiles, size = hard_hbm.shape
    rows_all = vec_ref.shape[0] - 1

    def local_copies():
        return [
            pltpu.make_async_copy(source, local_ref.at[place], local_sems.at[place])
            for place, source in enumerate((hard_hbm, soft_hbm, link_hbm))
        ]

    list_copy = pltpu.make_async_copy(list_hbm, list_ref, local_sems.at[3])
    list_copy.start()
    for copy in local_copies():
        copy.start()

    field = lax.broadcasted_iota(jnp.int32, (8, size), 0)
    scale = jnp.where(field < 4, jnp.float32(length_scale), jnp.float32(width_scale))

    def prepare(tile, carry):
        row_ref[tile] = joined_ref[pl.ds(tile, 8, stride=rows_all), :] * scale
        return carry

    lax.fori_loop(0, rows_all, prepare, 0, unroll=8)
    row_ref[rows_all] = jnp.ones((8, size), jnp.float32)
    fill_vectors(joined_ref, 5 * rows_all, rows_all, vec_ref)

    atom = lax.broadcasted_iota(jnp.int32, (size, size), 0)
    partner_atom = lax.broadcasted_iota(jnp.int32, (size, size), 1)
    apart_ref[...] = jnp.where(atom == partner_atom, jnp.inf, 0.0).astype(jnp.float32)

    line = lax.broadcasted_iota(jnp.int32, (32, 5 * size), 0)
    chosen = lax.broadcasted_iota(jnp.int32, (32, 5 * size), 1) // size
    select = jnp.where(((line & 7) == chosen) & (line < 24), 1.0, 0.0).astype(jnp.bfloat16)

    def spread(tile, carry):
        params = row_ref[tile]
        stacked = jnp.concatenate(split_rows(params) + [jnp.zeros_like(params)], axis=0)
        spread_ref[tile] = lax.dot_general(
            stacked.astype(jnp.bfloat16), select, (((0,), (0,)), ((), ())), preferred_element_type=jnp.float32)
        sum_ref[tile] = jnp.zeros(sum_ref.shape[1:], jnp.float32)
        return carry

    lax.fori_loop(0, tiles, spread, 0, unroll=8)
    sum_ref[tiles] = jnp.zeros(sum_ref.shape[1:], jnp.float32)

    def multiply(ring_ref, base, entries, kind):
        blocks = [lambda place=place: ring_ref[base, place] for place in range(BUILD_PAIRS)]
        add_products(vec_ref, sum_ref, blocks, entries, kind)

    def out_copy(ring_ref, half, base, first):
        return pltpu.make_async_copy(
            ring_ref.at[base], store_ref.at[pl.ds(first, BUILD_PAIRS)], sems.at[half, base])

    def pair_block(ring_ref, base, slot, entry, own_pairs):
        own = jnp.minimum(own_of(entry), tiles - 1)
        partner = partner_of(entry)
        place, lanes = slot // 2, slice(slot % 2 * size, slot % 2 * size + size)
        shift_a = (((entry >> 8) & 3) - 1).astype(jnp.float32) * length_scale
        shift_b = (((entry >> 10) & 3) - 1).astype(jnp.float32) * length_scale
        shift_c = (((entry >> 12) & 3) - 1).astype(jnp.float32) * length_scale
        theirs = row_ref[partner]
        full = (16, size)
        their_a = jnp.broadcast_to(theirs[0:1] + shift_a, full)
        their_b = jnp.broadcast_to(theirs[1:2] + shift_b, full)
        their_c = jnp.broadcast_to(theirs[2:3] + shift_c, full)
        their_shield = jnp.broadcast_to(theirs[3:4], full)
        their_width = jnp.broadcast_to(theirs[4:5], full)
        for group in range(size // 16):
            rows = slice(16 * group, 16 * group + 16)

            def mine(c):
                return spread_ref[own, rows, c * size : (c + 1) * size]

            delta_a = their_a - mine(0)
            delta_b = their_b - mine(1)
            delta_c = their_c - mine(2)
            distance = delta_a * delta_a + delta_b * delta_b + delta_c * delta_c
            if own_pairs:
                distance = distance + apart_ref[rows, :]
            coulomb = lax.rsqrt(distance + mine(3) * their_shield)
            response = response_scale * jnp.exp2(distance / (mine(4) + their_width))
            ring_ref[base, place, rows, lanes] = coulomb.astype(jnp.bfloat16)
            ring_ref[base, place, size + 16 * group : size + 16 * group + 16, lanes] = response.astype(jnp.bfloat16)

    def entries_at(first):
        return [list_ref[first + slot] for slot in range(BUILD_SLOTS)]

    def turns(first, last, kind):
        def visit(turn, carry):
            base = lax.rem(turn, BUILD_RING)
            before = lax.rem(turn + BUILD_RING - 1, BUILD_RING)
            start = turn * TURN

            @pl.when(turn >= BUILD_RING)
            def _():
                out_copy(even_ref, 0, base, 0).wait()
                out_copy(odd_ref, 1, base, 0).wait()

            late = [
                jnp.where(turn > first, list_ref[jnp.maximum(start - BUILD_SLOTS + slot, 0)], nothing)
                for slot in range(BUILD_SLOTS)
            ]
            even, odd = entries_at(start), entries_at(start + BUILD_SLOTS)
            multiply(odd_ref, before, late, kind)
            for slot, entry in enumerate(even):
                pair_block(even_ref, base, slot, entry, kind == "own")
            multiply(even_ref, base, even, kind)
            for slot, entry in enumerate(odd):
                pair_block(odd_ref, base, slot, entry, kind == "own")
            out_copy(even_ref, 0, base, 2 * BUILD_PAIRS * turn).start()
            out_copy(odd_ref, 1, base, 2 * BUILD_PAIRS * turn + BUILD_PAIRS).start()
            return carry

        lax.fori_loop(first, last, visit, 0)

        @pl.when(last > first)
        def _():
            final = last - 1
            multiply(odd_ref, lax.rem(final, BUILD_RING), entries_at(final * TURN + BUILD_SLOTS), kind)

    nothing = packed(tiles, rows_all)
    assert tiles % TURN == 0
    own_turns = tiles // TURN
    list_copy.wait()
    halo_turns = list_ref[list_ref.shape[0] - 2]
    all_turns = list_ref[list_ref.shape[0] - 1]
    turns(0, jnp.minimum(halo_turns, own_turns), "own")
    turns(own_turns, halo_turns, "halo")
    turns(halo_turns, all_turns, "inner")
    for group in range(BUILD_RING):
        @pl.when(group < all_turns)
        def _():
            out_copy(even_ref, 0, group, 0).wait()
            out_copy(odd_ref, 1, group, 0).wait()

    for copy in local_copies():
        copy.wait()

    def finish(tile, carry):
        total = sum_ref[tile]
        one = pl.ds(tile, 1)
        diag_charge = local_ref[0, one, :] + total[12:13, 0:128] - SHIFT
        diag_potential = local_ref[1, one, :] + total[12:13, 128:256] - SHIFT
        linking = local_ref[2, one, :]
        diag_ref[0, one, :] = diag_charge
        diag_ref[1, one, :] = diag_potential
        diag_ref[2, one, :] = linking
        values = joined_ref[pl.ds(5 * rows_all + tile, 4, stride=rows_all), :]
        pair_charge, pair_potential = pair_parts(total)
        image_ref[pl.ds(tile, 4, stride=tiles), :] = image_rows(
            values, pair_charge, pair_potential, diag_charge, diag_potential, linking)
        return carry

    lax.fori_loop(0, tiles, finish, 0, unroll=4)


def apply_kernel(*refs):
    list_hbm, joined_ref, diag_hbm, store_ref = refs[:4]
    last = len(refs) > 12
    earlier_hbm = refs[4:6] if last else ()
    image_ref = refs[4 + len(earlier_hbm)]
    moment_ref = refs[7] if last else None
    vec_ref, sum_ref, ring_ref, diag_ref, list_ref = refs[8:13] if last else refs[5:10]
    earlier_refs = refs[13:15] if last else ()
    sems, local_sems = refs[-2:]

    tiles = diag_hbm.shape[1]
    rows_all = vec_ref.shape[0] - 1
    own_turns = tiles // TURN

    def in_copy(turn, first=0, places=TURN // 2):
        slot = lax.rem(turn, APPLY_RING)
        return pltpu.make_async_copy(
            store_ref.at[pl.ds(turn * (TURN // 2) + first, places)],
            ring_ref.at[slot, pl.ds(first, places)], sems.at[slot])

    def start_copies(turn):
        for first in range(0, TURN // 2, APPLY_COPY):
            in_copy(turn, first, APPLY_COPY).start()

    def local_copies():
        pairs = [(diag_hbm, diag_ref)] + list(zip(earlier_hbm, earlier_refs))
        return [
            pltpu.make_async_copy(source, target, local_sems.at[place])
            for place, (source, target) in enumerate(pairs)
        ]

    ahead = APPLY_RING - APPLY_MERGE
    list_copy = pltpu.make_async_copy(list_hbm, list_ref, local_sems.at[len(earlier_hbm) + 1])
    list_copy.start()
    for turn in range(min(ahead, own_turns)):
        start_copies(jnp.int32(turn))
    for copy in local_copies():
        copy.start()

    fill_vectors(joined_ref, 0, rows_all, vec_ref)

    def clear(tile, carry):
        sum_ref[tile] = jnp.zeros(sum_ref.shape[1:], jnp.float32)
        return carry

    lax.fori_loop(0, tiles + 1, clear, 0, unroll=4)

    list_copy.wait()
    halo_turns = list_ref[list_ref.shape[0] - 2]
    all_turns = list_ref[list_ref.shape[0] - 1]
    for turn in range(own_turns, ahead):
        @pl.when(turn < all_turns)
        def _():
            start_copies(jnp.int32(turn))

    def visits(first, last, kind):
        def several(turn, merged):
            for step in range(merged):
                @pl.when(turn + step + ahead < all_turns)
                def _():
                    start_copies(turn + step + ahead)

            for step in range(merged):
                in_copy(turn + step).wait()
            entries = [list_ref[turn * TURN + place] for place in range(merged * TURN)]
            blocks = [
                lambda slot=lax.rem(turn + step, APPLY_RING), place=place: ring_ref[slot, place]
                for step in range(merged)
                for place in range(TURN // 2)
            ]
            add_products(vec_ref, sum_ref, blocks, entries, kind)

        def visit_many(group, carry):
            several(first + group * APPLY_MERGE, APPLY_MERGE)
            return carry

        def visit_one(turn, carry):
            several(turn, 1)
            return carry

        groups = (last - first) // APPLY_MERGE
        lax.fori_loop(0, groups, visit_many, 0)
        lax.fori_loop(first + groups * APPLY_MERGE, last, visit_one, 0)

    visits(0, jnp.minimum(halo_turns, own_turns), "own")
    visits(own_turns, halo_turns, "halo")
    visits(halo_turns, all_turns, "inner")
    for copy in local_copies():
        copy.wait()

    def finish(tile, carry):
        total = sum_ref[tile]
        one = pl.ds(tile, 1)
        values = joined_ref[pl.ds(tile, 4, stride=rows_all), :]
        pair_charge, pair_potential = pair_parts(total)
        image_ref[pl.ds(tile, 4, stride=tiles), :] = image_rows(
            values, pair_charge, pair_potential, diag_ref[0, one, :], diag_ref[1, one, :], diag_ref[2, one, :])
        return carry

    lax.fori_loop(0, tiles, finish, 0, unroll=4)

    if last:
        lane = lax.broadcasted_iota(jnp.int32, (1, 128), 1)

        def rows_of(order, field):
            if order == 2:
                return joined_ref[field * rows_all : field * rows_all + tiles, :]
            ref = (earlier_refs[0], earlier_refs[1], None, image_ref)[order]
            return ref[field * tiles : (field + 1) * tiles, :]

        lines = []
        for system in range(2):
            line = jnp.zeros((1, 128), jnp.float32)
            for degree in range(2 * ITERS):
                left, right = degree // 2, degree - degree // 2
                product = rows_of(left, system) * rows_of(right, system)
                product = product + rows_of(left, 2 + system) * rows_of(right, 2 + system)
                line = jnp.where(lane == degree, jnp.sum(product, keepdims=True), line)
            lines.append(line)
        both = jnp.concatenate(lines, axis=0)
        moment_ref[...] = jnp.broadcast_to(both[None], moment_ref.shape)


def combine_kernel(moments_ref, zero_ref, one_ref, two_ref, three_ref, solution_ref, residual_ref):
    tiles = zero_ref.shape[0] // 4
    total = jnp.sum(moments_ref[...], axis=0)
    moments = [total[:, degree : degree + 1] for degree in range(2 * ITERS)]

    def times(poly):
        grown = [SHIFT * c for c in poly] + [jnp.zeros_like(poly[0])]
        return [c + p for c, p in zip(grown, [jnp.zeros_like(poly[0])] + poly)]

    def product(left, right):
        out = 0.0
        for i, a in enumerate(left):
            for j, c in enumerate(right):
                out = out + a * c * moments[i + j]
        return out

    def axpy(left, scale, right):
        length = max(len(left), len(right))
        zero = jnp.zeros_like(scale)
        left = left + [zero] * (length - len(left))
        right = right + [zero] * (length - len(right))
        return [a + scale * c for a, c in zip(left, right)]

    one = jnp.ones_like(moments[0])
    found = [jnp.zeros_like(one)]
    rest = [one]
    direction = [one]
    norm = moments[0]
    for iteration in range(ITERS):
        along = times(direction)
        step = norm / product(direction, along)
        found = axpy(found, step, direction)
        rest = axpy(rest, -step, along)
        if iteration + 1 < ITERS:
            norm_next = product(rest, rest)
            direction = axpy(rest, norm_next / norm, direction)
            norm = norm_next
    refs = (zero_ref, one_ref, two_ref, three_ref)
    for field in range(4):
        system = field % 2
        span = slice(field * tiles, field * tiles + tiles)
        for poly, out_ref in ((found, solution_ref), (rest, residual_ref)):
            value = 0.0
            for c, ref in zip(poly, refs):
                value = value + c[system : system + 1, :] * ref[span, :]
            out_ref[span, :] = value


VMEM = pltpu.MemorySpace.VMEM
SMEM = pltpu.MemorySpace.SMEM


def in_vmem():
    return pl.BlockSpec(memory_space=VMEM)


def in_hbm():
    return pl.BlockSpec(memory_space=pltpu.MemorySpace.HBM)


def pinned(array):
    return pltpu.with_memory_space_constraint(array, pltpu.MemorySpace.HBM)


def in_smem():
    return pl.BlockSpec(memory_space=SMEM)


def on_device(positions, shield, width, hardness, softness, coupling, pair_bits, right_side):
    extent = hardness.shape[:3]
    size = hardness.shape[3]
    tiles = extent[0] * extent[1] * extent[2]
    counts = {axis: lax.axis_size(axis) for axis in AXES}
    f32 = jnp.float32

    hard, soft, link = (a.reshape(tiles, size) for a in (hardness, softness, coupling))
    start = right_side.reshape(4, tiles, size)
    fields = jnp.concatenate(
        [positions.reshape(3, tiles, size), shield.reshape(1, tiles, size), width.reshape(1, tiles, size), start],
        axis=0)
    joined, boxes = extended(fields, extent)
    rows_all = joined.shape[1]
    halo, inner = candidate_pairs(boxes, extent, counts)
    entries = tiles + sum(-(-len(found) // 2) * 2 for found in halo + inner)
    entries = -(-(entries + 3 * TURN) // TURN) * TURN

    tables = [jnp.asarray(list_table(found, packed(tiles, rows_all))) for found in (halo, inner)]
    slots = pl.pallas_call(
        functools.partial(list_kernel, spare=rows_all),
        out_shape=jax.ShapeDtypeStruct((entries + 2,), jnp.int32),
        in_specs=[in_smem()] * 3,
        out_specs=in_smem(),
        scratch_shapes=[pltpu.SMEM((tiles,), jnp.int32)],
        name="pair_list",
    )(pair_bits, *tables)
    slots = pinned(slots)

    flat = (4 * tiles, size)
    start_flat = start.reshape(flat)
    store, diag, image = pl.pallas_call(
        build_kernel,
        out_shape=(
            jax.ShapeDtypeStruct((entries // 2, 2 * size, 2 * size), jnp.bfloat16),
            jax.ShapeDtypeStruct((3, tiles, size), f32),
            jax.ShapeDtypeStruct(flat, f32),
        ),
        in_specs=[in_hbm(), in_vmem()] + [in_hbm()] * 3,
        out_specs=(in_hbm(), in_vmem(), in_vmem()),
        scratch_shapes=[
            pltpu.VMEM((rows_all + 1, 8, size), f32),
            pltpu.VMEM((tiles, size, 5 * size), f32),
            pltpu.VMEM((rows_all + 1, 16, size), jnp.bfloat16),
            pltpu.VMEM((tiles + 1, 16, 2 * size), f32),
            pltpu.VMEM((BUILD_RING, BUILD_PAIRS, 2 * size, 2 * size), jnp.bfloat16),
            pltpu.VMEM((BUILD_RING, BUILD_PAIRS, 2 * size, 2 * size), jnp.bfloat16),
            pltpu.VMEM((3, tiles, size), f32),
            pltpu.SMEM((entries + 2,), jnp.int32),
            pltpu.VMEM((size, size), f32),
            pltpu.SemaphoreType.DMA((2, BUILD_RING)),
            pltpu.SemaphoreType.DMA((4,)),
        ],
        compiler_params=pltpu.CompilerParams(vmem_limit_bytes=40 * 2**20),
        name="build",
    )(slots, joined.reshape(-1, size), pinned(hard), pinned(soft), pinned(link))

    devices = counts["gx"] * counts["gy"] * counts["gz"]
    diag = pinned(diag)

    def operate(vector, earlier=()):
        spread, _ = extended(vector.reshape(4, tiles, size), extent)
        last = len(earlier) > 0
        more = len(earlier)
        image_shape = jax.ShapeDtypeStruct(flat, f32)
        moment_shape = jax.ShapeDtypeStruct((devices, 2, size), f32)
        return pl.pallas_call(
            apply_kernel,
            out_shape=(image_shape, moment_shape) if last else image_shape,
            in_specs=[in_hbm(), in_vmem()] + [in_hbm()] * (2 + more),
            out_specs=(in_vmem(), in_vmem()) if last else in_vmem(),
            scratch_shapes=[
                pltpu.VMEM((rows_all + 1, 16, size), jnp.bfloat16),
                pltpu.VMEM((tiles + 1, 16, 2 * size), f32),
                pltpu.VMEM((APPLY_RING, TURN // 2, 2 * size, 2 * size), jnp.bfloat16),
                pltpu.VMEM((3, tiles, size), f32),
                pltpu.SMEM((entries + 2,), jnp.int32),
            ] + [pltpu.VMEM(flat, f32)] * more + [
                pltpu.SemaphoreType.DMA((APPLY_RING,)),
                pltpu.SemaphoreType.DMA((2 + more,)),
            ],
            compiler_params=pltpu.CompilerParams(vmem_limit_bytes=40 * 2**20),
            name="apply_last" if last else "apply",
        )(slots, spread.reshape(-1, size), diag, store, *[pinned(v) for v in earlier])

    second = operate(image)
    third, moments = operate(second, (start_flat, image))
    vectors = (start_flat, image, second, third)
    gathered = lax.all_to_all(moments, AXES, 0, 0)
    solution, residual = pl.pallas_call(
        combine_kernel,
        out_shape=(jax.ShapeDtypeStruct(flat, f32), jax.ShapeDtypeStruct(flat, f32)),
        in_specs=[in_vmem()] * 5,
        out_specs=(in_vmem(), in_vmem()),
        name="combine",
    )(gathered, *vectors)
    return (solution.reshape(right_side.shape), residual.reshape(right_side.shape))


def solution(mesh):
    return jax.shard_map(
        on_device,
        mesh=mesh,
        in_specs=(
            P(None, "gx", "gy", "gz", None),
            P("gx", "gy", "gz", None),
            P("gx", "gy", "gz", None),
            P("gx", "gy", "gz", None),
            P("gx", "gy", "gz", None),
            P("gx", "gy", "gz", None),
            P("gx", "gy", "gz"),
            P(None, "gx", "gy", "gz", None),
        ),
        out_specs=(P(None, "gx", "gy", "gz", None), P(None, "gx", "gy", "gz", None)),
        check_vma=False,
    )
```

```python
import functools
import math

import jax
import jax.numpy as jnp
import numpy as np
from jax import lax
from jax.experimental import pallas as pl
from jax.experimental.pallas import tpu as pltpu
from jax.sharding import PartitionSpec as P

ITERS = 3

coulomb_scale = 0.002
response_scale = 0.003
length_scale = 1.0 / coulomb_scale
width_scale = -math.log(2.0) * length_scale * length_scale

SHIFT = 3.0

AXES = ("gx", "gy", "gz")
HALO_ORDER = (("gy", 1), ("gx", 0), ("gz", 2))
PARTS = 3
TURN_BITS = 3
TURN = 1 << TURN_BITS
BUILD_SLOTS = TURN // 2
BUILD_PAIRS = BUILD_SLOTS // 2
BUILD_RING = 8
APPLY_COPY = 1
APPLY_RING = 12
APPLY_MERGE = 3


class Piece:
    def __init__(self, array, boxes):
        self.array = array
        self.boxes = boxes

    def face(self, dim, level):
        rows, boxes = [], []
        offset = 0
        for origin, shape in self.boxes:
            volume = shape[0] * shape[1] * shape[2]
            if origin[dim] <= level < origin[dim] + shape[dim]:
                part = self.array[:, offset : offset + volume]
                part = part.reshape((part.shape[0],) + shape + part.shape[2:])
                part = lax.slice_in_dim(part, level - origin[dim], level - origin[dim] + 1, axis=dim + 1)
                cut = tuple(1 if d == dim else shape[d] for d in range(3))
                rows.append(part.reshape(part.shape[0], -1, part.shape[-1]))
                boxes.append((tuple(level if d == dim else origin[d] for d in range(3)), cut))
            offset += volume
        return rows, boxes


def whole_face(pieces, dim, level):
    rows, boxes = [], []
    for piece in pieces:
        more_rows, more_boxes = piece.face(dim, level)
        rows += more_rows
        boxes += more_boxes
    return (jnp.concatenate(rows, axis=1) if len(rows) > 1 else rows[0]), boxes


def moved(boxes, dim, level):
    return [(tuple(level if d == dim else o[d] for d in range(3)), s) for o, s in boxes]


def extended(block, extent):
    pieces = [Piece(block, [((0, 0, 0), extent)])]
    for axis, dim in HALO_ORDER:
        count = lax.axis_size(axis)
        if count == 1:
            continue
        size = extent[dim]
        first, boxes = whole_face(pieces, dim, 0)
        last, _ = whole_face(pieces, dim, size - 1)
        if count == 2:
            sent = jnp.where(lax.axis_index(axis) == 0, last, first)
            got = lax.ppermute(sent, axis, [(0, 1), (1, 0)])
            pieces = pieces + [Piece(got, moved(boxes, dim, size))]
        else:
            forward = [(i, (i + 1) % count) for i in range(count)]
            backward = [(target, source) for source, target in forward]
            low = lax.ppermute(last, axis, forward)
            high = lax.ppermute(first, axis, backward)
            pieces = pieces + [
                Piece(low, moved(boxes, dim, -1)),
                Piece(high, moved(boxes, dim, size)),
            ]
    joined = jnp.concatenate([piece.array for piece in pieces], axis=1)
    return joined, [box for piece in pieces for box in piece.boxes]


def storage_rows(boxes, extent, counts):
    rows = {}
    offset = 0
    for origin, shape in boxes:
        for a in range(shape[0]):
            for b in range(shape[1]):
                for c in range(shape[2]):
                    rows[(origin[0] + a, origin[1] + b, origin[2] + c)] = offset
                    offset += 1

    def row_of(coord):
        fixed = list(coord)
        for axis, dim in HALO_ORDER:
            outside = not 0 <= fixed[dim] < extent[dim]
            if outside and counts[axis] == 1:
                fixed[dim] = 0
            elif outside and counts[axis] == 2:
                fixed[dim] = extent[dim]
        return rows[tuple(fixed)]

    return row_of


def candidate_pairs(boxes, extent, counts):
    row_of = storage_rows(boxes, extent, counts)
    tiles = extent[0] * extent[1] * extent[2]
    halo, inner = [], []
    for x in range(extent[0]):
        for y in range(extent[1]):
            for z in range(extent[2]):
                own = (x * extent[1] + y) * extent[2] + z
                halo.append([])
                inner.append([])
                for code in range(27):
                    a, b, c = code // 9, code // 3 % 3, code % 3
                    partner = row_of((x + a - 1, y + b - 1, z + c - 1))
                    assert own < 255 and partner < 255
                    entry = packed(own, partner, a, b, c)
                    if partner >= tiles:
                        halo[-1].append((code, entry))
                    elif partner > own:
                        inner[-1].append((code, entry))
    return halo, inner


def packed(own, partner, a=1, b=1, c=1):
    return own | a << 8 | b << 10 | c << 12 | partner << 14


def own_of(entry):
    return entry & 255


def partner_of(entry):
    return (entry >> 14) & 255


def list_table(found_of, never):
    longest = max(len(found) for found in found_of)
    table = [
        [entry | code << 22 for code, entry in found] + [never | 31 << 22] * (longest - len(found))
        for found in found_of
    ]
    return np.asarray([entry - (1 << 32) if entry >> 31 else entry for row in table for entry in row], np.int32)


def list_kernel(bits_ref, halo_ref, inner_ref, list_ref, word_ref, *, spare):
    height, depth = bits_ref.shape[1:]
    tiles = word_ref.shape[0]
    for tile in range(tiles):
        list_ref[tile] = jnp.int32(packed(tile, tile))
        word_ref[tile] = bits_ref[tile // (height * depth), tile // depth % height, tile % depth]
    filled = jnp.int32(tiles)
    for part, table_ref in enumerate((halo_ref, inner_ref)):
        longest = table_ref.shape[0] // tiles

        def visit(tile, filled):
            word = word_ref[tile]
            for place in range(longest):
                entry = table_ref[tile * longest + place]
                list_ref[filled] = entry
                filled = filled + ((word >> ((entry >> 22) & 31)) & 1)
            list_ref[filled] = tile | packed(0, spare)
            return filled + (filled & 1)

        filled = lax.fori_loop(0, tiles, visit, filled)

        def pad(extra, carry):
            list_ref[filled + extra] = jnp.int32(packed(tiles, spare))
            return carry

        lax.fori_loop(0, TURN, pad, 0)
        filled = (filled + TURN - 1) & -TURN
        list_ref[list_ref.shape[0] - 2 + part] = filled >> TURN_BITS


def split_rows(values):
    parts = []
    rest = values
    for _ in range(PARTS):
        part = rest.astype(jnp.bfloat16).astype(jnp.float32)
        parts.append(part)
        rest = rest - part
    return parts


def fill_vectors(source_ref, first_row, rows_all, vec_ref):
    vec_ref[rows_all] = jnp.zeros(vec_ref.shape[1:], jnp.bfloat16)

    def one(tile, carry):
        values = source_ref[pl.ds(first_row + tile, 4, stride=rows_all), :]
        parts = split_rows(values)
        stacked = jnp.concatenate(parts + [jnp.ones_like(values)], axis=0)
        vec_ref[tile] = stacked.astype(jnp.bfloat16)
        return carry

    lax.fori_loop(0, rows_all, one, 0, unroll=8)


def pair_parts(total):
    joined = total[0:4] + total[4:8] + total[8:12]
    return joined[0:2, 0:128], joined[2:4, 128:256]


def image_rows(values, pair_charge, pair_potential, diag_charge, diag_potential, linking):
    charge, potential = values[0:2], values[2:4]
    image_charge = diag_charge * charge + pair_charge + linking * potential
    image_potential = diag_potential * potential - pair_potential + linking * charge
    return jnp.concatenate([image_charge, image_potential], axis=0)


def add_products(vec_ref, sum_ref, blocks, entries, kind):
    spare_sum = sum_ref.shape[0] - 1
    added = []

    def times(vectors, block):
        return jnp.dot(vectors, block, preferred_element_type=jnp.float32)

    for place, block in enumerate(blocks):
        pair = entries[2 * place : 2 * place + 2]
        half = block().shape[0] // 2
        if kind == "own":
            for side, entry in enumerate(pair):
                vectors = vec_ref[own_of(entry)]
                lanes = slice(side * half, side * half + half)
                added.append((own_of(entry), lax.dot_general(
                    vectors, block()[:, lanes], (((1,), (1,)), ((), ())), preferred_element_type=jnp.float32)))
            continue
        vectors = jnp.concatenate([vec_ref[partner_of(entry)] for entry in pair], axis=1)
        added.append((own_of(pair[0]), lax.dot_general(
            vectors, block(), (((1,), (1,)), ((), ())), preferred_element_type=jnp.float32)))
        if kind == "inner":
            vectors = vec_ref[own_of(pair[0])]
            coulomb, response = times(vectors, block()[:half]), times(vectors, block()[half:])
            for side, entry in enumerate(pair):
                lanes = slice(side * half, side * half + half)
                added.append((
                    jnp.minimum(partner_of(entry), spare_sum),
                    jnp.concatenate([coulomb[:, lanes], response[:, lanes]], axis=1)))
    for tile, product in added:
        sum_ref[tile] = sum_ref[tile] + product


def build_kernel(list_hbm, joined_ref, hard_hbm, soft_hbm, link_hbm,
                 store_ref, diag_ref, image_ref,
                 row_ref, spread_ref, vec_ref, sum_ref, even_ref, odd_ref,
                 local_ref, list_ref, apart_ref, sems, local_sems):
    tiles, size = hard_hbm.shape
    rows_all = vec_ref.shape[0] - 1

    def local_copies():
        return [
            pltpu.make_async_copy(source, local_ref.at[place], local_sems.at[place])
            for place, source in enumerate((hard_hbm, soft_hbm, link_hbm))
        ]

    list_copy = pltpu.make_async_copy(list_hbm, list_ref, local_sems.at[3])
    list_copy.start()
    for copy in local_copies():
        copy.start()

    field = lax.broadcasted_iota(jnp.int32, (8, size), 0)
    scale = jnp.where(field < 4, jnp.float32(length_scale), jnp.float32(width_scale))

    def prepare(tile, carry):
        row_ref[tile] = joined_ref[pl.ds(tile, 8, stride=rows_all), :] * scale
        return carry

    lax.fori_loop(0, rows_all, prepare, 0, unroll=8)
    row_ref[rows_all] = jnp.ones((8, size), jnp.float32)
    fill_vectors(joined_ref, 5 * rows_all, rows_all, vec_ref)

    atom = lax.broadcasted_iota(jnp.int32, (size, size), 0)
    partner_atom = lax.broadcasted_iota(jnp.int32, (size, size), 1)
    apart_ref[...] = jnp.where(atom == partner_atom, jnp.inf, 0.0).astype(jnp.float32)

    line = lax.broadcasted_iota(jnp.int32, (32, 5 * size), 0)
    chosen = lax.broadcasted_iota(jnp.int32, (32, 5 * size), 1) // size
    select = jnp.where(((line & 7) == chosen) & (line < 24), 1.0, 0.0).astype(jnp.bfloat16)

    def spread(tile, carry):
        params = row_ref[tile]
        stacked = jnp.concatenate(split_rows(params) + [jnp.zeros_like(params)], axis=0)
        spread_ref[tile] = lax.dot_general(
            stacked.astype(jnp.bfloat16), select, (((0,), (0,)), ((), ())), preferred_element_type=jnp.float32)
        sum_ref[tile] = jnp.zeros(sum_ref.shape[1:], jnp.float32)
        return carry

    lax.fori_loop(0, tiles, spread, 0, unroll=8)
    sum_ref[tiles] = jnp.zeros(sum_ref.shape[1:], jnp.float32)

    def multiply(ring_ref, base, entries, kind):
        blocks = [lambda place=place: ring_ref[base, place] for place in range(BUILD_PAIRS)]
        add_products(vec_ref, sum_ref, blocks, entries, kind)

    def out_copy(ring_ref, half, base, first):
        return pltpu.make_async_copy(
            ring_ref.at[base], store_ref.at[pl.ds(first, BUILD_PAIRS)], sems.at[half, base])

    def pair_block(ring_ref, base, slot, entry, own_pairs):
        own = jnp.minimum(own_of(entry), tiles - 1)
        partner = partner_of(entry)
        place, lanes = slot // 2, slice(slot % 2 * size, slot % 2 * size + size)
        shift_a = (((entry >> 8) & 3) - 1).astype(jnp.float32) * length_scale
        shift_b = (((entry >> 10) & 3) - 1).astype(jnp.float32) * length_scale
        shift_c = (((entry >> 12) & 3) - 1).astype(jnp.float32) * length_scale
        theirs = row_ref[partner]
        full = (16, size)
        their_a = jnp.broadcast_to(theirs[0:1] + shift_a, full)
        their_b = jnp.broadcast_to(theirs[1:2] + shift_b, full)
        their_c = jnp.broadcast_to(theirs[2:3] + shift_c, full)
        their_shield = jnp.broadcast_to(theirs[3:4], full)
        their_width = jnp.broadcast_to(theirs[4:5], full)
        for group in range(size // 16):
            rows = slice(16 * group, 16 * group + 16)

            def mine(c):
                return spread_ref[own, rows, c * size : (c + 1) * size]

            delta_a = their_a - mine(0)
            delta_b = their_b - mine(1)
            delta_c = their_c - mine(2)
            distance = delta_a * delta_a + delta_b * delta_b + delta_c * delta_c
            if own_pairs:
                distance = distance + apart_ref[rows, :]
            coulomb = lax.rsqrt(distance + mine(3) * their_shield)
            response = response_scale * jnp.exp2(distance / (mine(4) + their_width))
            ring_ref[base, place, rows, lanes] = coulomb.astype(jnp.bfloat16)
            ring_ref[base, place, size + 16 * group : size + 16 * group + 16, lanes] = response.astype(jnp.bfloat16)

    def entries_at(first):
        return [list_ref[first + slot] for slot in range(BUILD_SLOTS)]

    def turns(first, last, kind):
        def visit(turn, carry):
            base = lax.rem(turn, BUILD_RING)
            before = lax.rem(turn + BUILD_RING - 1, BUILD_RING)
            start = turn * TURN

            @pl.when(turn >= BUILD_RING)
            def _():
                out_copy(even_ref, 0, base, 0).wait()
                out_copy(odd_ref, 1, base, 0).wait()

            late = [
                jnp.where(turn > first, list_ref[jnp.maximum(start - BUILD_SLOTS + slot, 0)], nothing)
                for slot in range(BUILD_SLOTS)
            ]
            even, odd = entries_at(start), entries_at(start + BUILD_SLOTS)
            multiply(odd_ref, before, late, kind)
            for slot, entry in enumerate(even):
                pair_block(even_ref, base, slot, entry, kind == "own")
            multiply(even_ref, base, even, kind)
            for slot, entry in enumerate(odd):
                pair_block(odd_ref, base, slot, entry, kind == "own")
            out_copy(even_ref, 0, base, 2 * BUILD_PAIRS * turn).start()
            out_copy(odd_ref, 1, base, 2 * BUILD_PAIRS * turn + BUILD_PAIRS).start()
            return carry

        lax.fori_loop(first, last, visit, 0)

        @pl.when(last > first)
        def _():
            final = last - 1
            multiply(odd_ref, lax.rem(final, BUILD_RING), entries_at(final * TURN + BUILD_SLOTS), kind)

    nothing = packed(tiles, rows_all)
    assert tiles % TURN == 0
    own_turns = tiles // TURN
    list_copy.wait()
    halo_turns = list_ref[list_ref.shape[0] - 2]
    all_turns = list_ref[list_ref.shape[0] - 1]
    turns(0, jnp.minimum(halo_turns, own_turns), "own")
    turns(own_turns, halo_turns, "halo")
    turns(halo_turns, all_turns, "inner")
    for group in range(BUILD_RING):
        @pl.when(group < all_turns)
        def _():
            out_copy(even_ref, 0, group, 0).wait()
            out_copy(odd_ref, 1, group, 0).wait()

    for copy in local_copies():
        copy.wait()

    def finish(tile, carry):
        total = sum_ref[tile]
        one = pl.ds(tile, 1)
        diag_charge = local_ref[0, one, :] + total[12:13, 0:128] - SHIFT
        diag_potential = local_ref[1, one, :] + total[12:13, 128:256] - SHIFT
        linking = local_ref[2, one, :]
        diag_ref[0, one, :] = diag_charge
        diag_ref[1, one, :] = diag_potential
        diag_ref[2, one, :] = linking
        values = joined_ref[pl.ds(5 * rows_all + tile, 4, stride=rows_all), :]
        pair_charge, pair_potential = pair_parts(total)
        image_ref[pl.ds(tile, 4, stride=tiles), :] = image_rows(
            values, pair_charge, pair_potential, diag_charge, diag_potential, linking)
        return carry

    lax.fori_loop(0, tiles, finish, 0, unroll=8)


def apply_kernel(*refs):
    list_hbm, joined_ref, diag_hbm, store_ref = refs[:4]
    last = len(refs) > 12
    earlier_hbm = refs[4:6] if last else ()
    image_ref = refs[4 + len(earlier_hbm)]
    moment_ref = refs[7] if last else None
    vec_ref, sum_ref, ring_ref, diag_ref, list_ref = refs[8:13] if last else refs[5:10]
    earlier_refs = refs[13:15] if last else ()
    sems, local_sems = refs[-2:]

    tiles = diag_hbm.shape[1]
    rows_all = vec_ref.shape[0] - 1
    own_turns = tiles // TURN

    def in_copy(turn, first=0, places=TURN // 2):
        slot = lax.rem(turn, APPLY_RING)
        return pltpu.make_async_copy(
            store_ref.at[pl.ds(turn * (TURN // 2) + first, places)],
            ring_ref.at[slot, pl.ds(first, places)], sems.at[slot])

    def start_copies(turn):
        for first in range(0, TURN // 2, APPLY_COPY):
            in_copy(turn, first, APPLY_COPY).start()

    def local_copies():
        pairs = [(diag_hbm, diag_ref)] + list(zip(earlier_hbm, earlier_refs))
        return [
            pltpu.make_async_copy(source, target, local_sems.at[place])
            for place, (source, target) in enumerate(pairs)
        ]

    ahead = APPLY_RING - APPLY_MERGE
    list_copy = pltpu.make_async_copy(list_hbm, list_ref, local_sems.at[len(earlier_hbm) + 1])
    list_copy.start()
    for turn in range(min(ahead, own_turns)):
        start_copies(jnp.int32(turn))
    for copy in local_copies():
        copy.start()

    fill_vectors(joined_ref, 0, rows_all, vec_ref)

    def clear(tile, carry):
        sum_ref[tile] = jnp.zeros(sum_ref.shape[1:], jnp.float32)
        return carry

    lax.fori_loop(0, tiles + 1, clear, 0, unroll=4)

    list_copy.wait()
    halo_turns = list_ref[list_ref.shape[0] - 2]
    all_turns = list_ref[list_ref.shape[0] - 1]
    for turn in range(own_turns, ahead):
        @pl.when(turn < all_turns)
        def _():
            start_copies(jnp.int32(turn))

    def visits(first, last, kind):
        def several(turn, merged):
            for step in range(merged):
                @pl.when(turn + step + ahead < all_turns)
                def _():
                    start_copies(turn + step + ahead)

            for step in range(merged):
                in_copy(turn + step).wait()
            entries = [list_ref[turn * TURN + place] for place in range(merged * TURN)]
            blocks = [
                lambda slot=lax.rem(turn + step, APPLY_RING), place=place: ring_ref[slot, place]
                for step in range(merged)
                for place in range(TURN // 2)
            ]
            add_products(vec_ref, sum_ref, blocks, entries, kind)

        def visit_many(group, carry):
            several(first + group * APPLY_MERGE, APPLY_MERGE)
            return carry

        def visit_one(turn, carry):
            several(turn, 1)
            return carry

        groups = (last - first) // APPLY_MERGE
        lax.fori_loop(0, groups, visit_many, 0)
        lax.fori_loop(first + groups * APPLY_MERGE, last, visit_one, 0)

    visits(0, jnp.minimum(halo_turns, own_turns), "own")
    visits(own_turns, halo_turns, "halo")
    visits(halo_turns, all_turns, "inner")
    for copy in local_copies():
        copy.wait()

    def finish(tile, carry):
        total = sum_ref[tile]
        one = pl.ds(tile, 1)
        values = joined_ref[pl.ds(tile, 4, stride=rows_all), :]
        pair_charge, pair_potential = pair_parts(total)
        image_ref[pl.ds(tile, 4, stride=tiles), :] = image_rows(
            values, pair_charge, pair_potential, diag_ref[0, one, :], diag_ref[1, one, :], diag_ref[2, one, :])
        return carry

    lax.fori_loop(0, tiles, finish, 0, unroll=8)

    if last:
        lane = lax.broadcasted_iota(jnp.int32, (1, 128), 1)

        def rows_of(order, field):
            if order == 2:
                return joined_ref[field * rows_all : field * rows_all + tiles, :]
            ref = (earlier_refs[0], earlier_refs[1], None, image_ref)[order]
            return ref[field * tiles : (field + 1) * tiles, :]

        lines = []
        for system in range(2):
            line = jnp.zeros((1, 128), jnp.float32)
            for degree in range(2 * ITERS):
                left, right = degree // 2, degree - degree // 2
                product = rows_of(left, system) * rows_of(right, system)
                product = product + rows_of(left, 2 + system) * rows_of(right, 2 + system)
                line = jnp.where(lane == degree, jnp.sum(product, keepdims=True), line)
            lines.append(line)
        both = jnp.concatenate(lines, axis=0)
        moment_ref[...] = jnp.broadcast_to(both[None], moment_ref.shape)


def combine_kernel(moments_ref, zero_ref, one_ref, two_ref, three_ref, solution_ref, residual_ref):
    tiles = zero_ref.shape[0] // 4
    total = jnp.sum(moments_ref[...], axis=0)
    moments = [total[:, degree : degree + 1] for degree in range(2 * ITERS)]

    def times(poly):
        grown = [SHIFT * c for c in poly] + [jnp.zeros_like(poly[0])]
        return [c + p for c, p in zip(grown, [jnp.zeros_like(poly[0])] + poly)]

    def product(left, right):
        out = 0.0
        for i, a in enumerate(left):
            for j, c in enumerate(right):
                out = out + a * c * moments[i + j]
        return out

    def axpy(left, scale, right):
        length = max(len(left), len(right))
        zero = jnp.zeros_like(scale)
        left = left + [zero] * (length - len(left))
        right = right + [zero] * (length - len(right))
        return [a + scale * c for a, c in zip(left, right)]

    one = jnp.ones_like(moments[0])
    found = [jnp.zeros_like(one)]
    rest = [one]
    direction = [one]
    norm = moments[0]
    for iteration in range(ITERS):
        along = times(direction)
        step = norm / product(direction, along)
        found = axpy(found, step, direction)
        rest = axpy(rest, -step, along)
        if iteration + 1 < ITERS:
            norm_next = product(rest, rest)
            direction = axpy(rest, norm_next / norm, direction)
            norm = norm_next
    refs = (zero_ref, one_ref, two_ref, three_ref)
    for field in range(4):
        system = field % 2
        span = slice(field * tiles, field * tiles + tiles)
        for poly, out_ref in ((found, solution_ref), (rest, residual_ref)):
            value = 0.0
            for c, ref in zip(poly, refs):
                value = value + c[system : system + 1, :] * ref[span, :]
            out_ref[span, :] = value


VMEM = pltpu.MemorySpace.VMEM
SMEM = pltpu.MemorySpace.SMEM


def in_vmem():
    return pl.BlockSpec(memory_space=VMEM)


def in_hbm():
    return pl.BlockSpec(memory_space=pltpu.MemorySpace.HBM)


def pinned(array):
    return pltpu.with_memory_space_constraint(array, pltpu.MemorySpace.HBM)


def in_smem():
    return pl.BlockSpec(memory_space=SMEM)


def on_device(positions, shield, width, hardness, softness, coupling, pair_bits, right_side):
    extent = hardness.shape[:3]
    size = hardness.shape[3]
    tiles = extent[0] * extent[1] * extent[2]
    counts = {axis: lax.axis_size(axis) for axis in AXES}
    f32 = jnp.float32

    hard, soft, link = (a.reshape(tiles, size) for a in (hardness, softness, coupling))
    start = right_side.reshape(4, tiles, size)
    fields = jnp.concatenate(
        [positions.reshape(3, tiles, size), shield.reshape(1, tiles, size), width.reshape(1, tiles, size), start],
        axis=0)
    fields = lax.optimization_barrier(fields)
    joined, boxes = extended(fields, extent)
    rows_all = joined.shape[1]
    halo, inner = candidate_pairs(boxes, extent, counts)
    entries = tiles + sum(-(-len(found) // 2) * 2 for found in halo + inner)
    entries = -(-(entries + 3 * TURN) // TURN) * TURN

    tables = [jnp.asarray(list_table(found, packed(tiles, rows_all))) for found in (halo, inner)]
    slots = pl.pallas_call(
        functools.partial(list_kernel, spare=rows_all),
        out_shape=jax.ShapeDtypeStruct((entries + 2,), jnp.int32),
        in_specs=[in_smem()] * 3,
        out_specs=in_smem(),
        scratch_shapes=[pltpu.SMEM((tiles,), jnp.int32)],
        name="pair_list",
    )(pair_bits, *tables)
    slots = pinned(slots)

    flat = (4 * tiles, size)
    start_flat = start.reshape(flat)
    store, diag, image = pl.pallas_call(
        build_kernel,
        out_shape=(
            jax.ShapeDtypeStruct((entries // 2, 2 * size, 2 * size), jnp.bfloat16),
            jax.ShapeDtypeStruct((3, tiles, size), f32),
            jax.ShapeDtypeStruct(flat, f32),
        ),
        in_specs=[in_hbm(), in_vmem()] + [in_hbm()] * 3,
        out_specs=(in_hbm(), in_vmem(), in_vmem()),
        scratch_shapes=[
            pltpu.VMEM((rows_all + 1, 8, size), f32),
            pltpu.VMEM((tiles, size, 5 * size), f32),
            pltpu.VMEM((rows_all + 1, 16, size), jnp.bfloat16),
            pltpu.VMEM((tiles + 1, 16, 2 * size), f32),
            pltpu.VMEM((BUILD_RING, BUILD_PAIRS, 2 * size, 2 * size), jnp.bfloat16),
            pltpu.VMEM((BUILD_RING, BUILD_PAIRS, 2 * size, 2 * size), jnp.bfloat16),
            pltpu.VMEM((3, tiles, size), f32),
            pltpu.SMEM((entries + 2,), jnp.int32),
            pltpu.VMEM((size, size), f32),
            pltpu.SemaphoreType.DMA((2, BUILD_RING)),
            pltpu.SemaphoreType.DMA((4,)),
        ],
        compiler_params=pltpu.CompilerParams(vmem_limit_bytes=40 * 2**20),
        name="build",
    )(slots, joined.reshape(-1, size), pinned(hard), pinned(soft), pinned(link))

    devices = counts["gx"] * counts["gy"] * counts["gz"]
    diag = pinned(diag)

    def operate(vector, earlier=()):
        spread, _ = extended(vector.reshape(4, tiles, size), extent)
        last = len(earlier) > 0
        more = len(earlier)
        image_shape = jax.ShapeDtypeStruct(flat, f32)
        moment_shape = jax.ShapeDtypeStruct((devices, 2, size), f32)
        return pl.pallas_call(
            apply_kernel,
            out_shape=(image_shape, moment_shape) if last else image_shape,
            in_specs=[in_hbm(), in_vmem()] + [in_hbm()] * (2 + more),
            out_specs=(in_vmem(), in_vmem()) if last else in_vmem(),
            scratch_shapes=[
                pltpu.VMEM((rows_all + 1, 16, size), jnp.bfloat16),
                pltpu.VMEM((tiles + 1, 16, 2 * size), f32),
                pltpu.VMEM((APPLY_RING, TURN // 2, 2 * size, 2 * size), jnp.bfloat16),
                pltpu.VMEM((3, tiles, size), f32),
                pltpu.SMEM((entries + 2,), jnp.int32),
            ] + [pltpu.VMEM(flat, f32)] * more + [
                pltpu.SemaphoreType.DMA((APPLY_RING,)),
                pltpu.SemaphoreType.DMA((2 + more,)),
            ],
            compiler_params=pltpu.CompilerParams(vmem_limit_bytes=40 * 2**20),
            name="apply_last" if last else "apply",
        )(slots, spread.reshape(-1, size), diag, store, *[pinned(v) for v in earlier])

    second = operate(image)
    third, moments = operate(second, (start_flat, image))
    vectors = (start_flat, image, second, third)
    gathered = lax.all_to_all(moments, AXES, 0, 0)
    solution, residual = pl.pallas_call(
        combine_kernel,
        out_shape=(jax.ShapeDtypeStruct(flat, f32), jax.ShapeDtypeStruct(flat, f32)),
        in_specs=[in_vmem()] * 5,
        out_specs=(in_vmem(), in_vmem()),
        name="combine",
    )(gathered, *vectors)
    return (solution.reshape(right_side.shape), residual.reshape(right_side.shape))


def solution(mesh):
    return jax.shard_map(
        on_device,
        mesh=mesh,
        in_specs=(
            P(None, "gx", "gy", "gz", None),
            P("gx", "gy", "gz", None),
            P("gx", "gy", "gz", None),
            P("gx", "gy", "gz", None),
            P("gx", "gy", "gz", None),
            P("gx", "gy", "gz", None),
            P("gx", "gy", "gz"),
            P(None, "gx", "gy", "gz", None),
        ),
        out_specs=(P(None, "gx", "gy", "gz", None), P(None, "gx", "gy", "gz", None)),
        check_vma=False,
    )
```
